32 devices in a mesh: dom: 8 (over y, x, core), rep: 4 (over z).
Axes of the slice: x: 2, y: 2, z: 4, core: 2. Of those that a mesh axis runs over, the one named last changes fastest.
Arguments:
- hop_feats: bfloat16 [3, 65536, 128], P(None, ('dom', 'rep')), may hold values from -6 to 6
- adj_local: bfloat16 [512, 12, 128, 128], P(('dom', 'rep')), may hold values from -0.125 to 0.125
- local_cols: int32 [512, 12], P(('dom', 'rep')), may hold values from 0 to 15
- adj_halo: bfloat16 [512, 4, 128, 128], P(('dom', 'rep')), may hold values from -0.125 to 0.125
- halo_cols: int32 [512, 4], P(('dom', 'rep')), may hold values from 0 to 3
- boundary_rows: int32 [32, 512], P(('dom', 'rep')), may hold values from 0 to 2047
- train_ids: int32 [32, 2048], P(('dom', 'rep')), may hold values from 0 to 2047, as said below
- shuffle: int32 [32, 2048], P(('dom', 'rep')), may hold values from 0 to 2047, as said below
- labels: int32 [65536], P(('dom', 'rep')), may hold values from 0 to 171
- labelled: int32 [65536], P(('dom', 'rep')), may hold values from 0 to 1
- w_first: bfloat16 [512, 1024], P(None, 'rep'), may hold values from -1 to 1
- w_second: bfloat16 [1024, 172], P('rep'), may hold values from -2 to 2
Outputs:
- next_hop: bfloat16 [65536, 128], P(('dom', 'rep'))
- batch_loss: float32 [32, 32], P(('dom', 'rep'))
- grad_first: float32 [512, 1024], P('dom', 'rep')
- grad_second: float32 [1024, 172], P('rep')
The draws below stay inside these ranges and needn't reach their ends.
Inputs may be any that keep to these rules, and one draw needn't show every extreme that they name: `local_cols`: local tile indices of the partition's own row tiles. `halo_cols`: indices of received boundary tiles. `boundary_rows`: rows of the sending partition itself. `train_ids`: rows of the partition itself. `shuffle`: each row is a permutation of 0 .. 2047.
All inputs are finite; a program needn't handle non-finite values.
Results may differ from the reference program's by a relative error of at most 0.005.
The reference program's roundings to bfloat16 on the way count: a program that leaves them out, or rounds other values in their place, can miss the bound.
Values may be sent and summed in bfloat16 or wider, within the bound.
A program may use at most 128 MiB of HBM per device.

```python
import math
import jax
import jax.numpy as jnp
from jax import lax

D_FEAT = 128
HIDDEN_UNITS = 1024
CLASSES = 172
TILE = 128
RT = 16
KL = 12
KH = 4
HALO_TILES = 4
SLOTS = 2048
NODES = 65536
N_DOM = 8
N_REP = 4
DEVICES = 32


def slot_parts(key):
    train_ids = jax.random.randint(jax.random.fold_in(key, 11), (DEVICES, SLOTS), 0, RT * TILE)
    row_keys = jax.random.split(jax.random.fold_in(key, 12), DEVICES)
    shuffle = jax.vmap(lambda one_key: jax.random.permutation(one_key, SLOTS))(row_keys).astype(jnp.int32)
    return (train_ids.astype(jnp.int32), shuffle)


def draw_hop_feats(key, part):
    base = jnp.clip(jax.random.normal(jax.random.fold_in(key, 1), (3, NODES, D_FEAT), jnp.float32), -6.0, 6.0)
    return base.astype(jnp.bfloat16)


def draw_w_first(key, part):
    width = 4 * D_FEAT
    scale = 1.0 / math.sqrt(width)
    base = jnp.clip(jax.random.normal(jax.random.fold_in(key, 4), (width, HIDDEN_UNITS), jnp.float32), -6.0, 6.0) * scale
    return base.astype(jnp.bfloat16)


def draw_w_second(key, part):
    scale = 1.0 / math.sqrt(HIDDEN_UNITS)
    base = jnp.clip(jax.random.normal(jax.random.fold_in(key, 5), (HIDDEN_UNITS, CLASSES), jnp.float32), -6.0, 6.0) * scale
    return base.astype(jnp.bfloat16)


def draw_train_ids(key, part):
    return slot_parts(key)[0]


def draw_shuffle(key, part):
    return slot_parts(key)[1]


def draw_labelled(key, part):
    train_ids, shuffle = slot_parts(key)
    base = (jax.random.randint(jax.random.fold_in(key, 13), (NODES,), 0, 3) < 2).astype(jnp.int32)
    bases = jnp.arange(DEVICES, dtype=jnp.int32)[:, None] * (RT * TILE)
    order = bases + jnp.take_along_axis(train_ids, shuffle, axis=1)
    per = SLOTS // DEVICES
    batches = jnp.transpose(order.reshape(DEVICES, DEVICES, per), (1, 0, 2)).reshape(DEVICES, SLOTS)
    empty = jax.random.randint(jax.random.fold_in(key, 14), (2,), 0, DEVICES)
    cleared = batches[empty].reshape(-1)
    return base.at[cleared].set(0)


def touch_ends(entries, rng, least, largest):
    extent = entries.shape
    index_at = [jax.random.randint(jax.random.fold_in(rng, axis), (), 0, extent[axis]) for axis in range(len(extent))]
    entries = entries.at[tuple(index_at)].set(least)
    longest = extent.index(max(extent))
    index_at[longest] = (index_at[longest] + 1) % extent[longest]
    return entries.at[tuple(index_at)].set(largest)


def steps_of(rng, dims, pieces, least, largest):
    def one(axis_at, parts):
        draws = jax.random.uniform(jax.random.fold_in(jax.random.fold_in(rng, 6), axis_at), (parts,), jnp.float32, least / len(pieces), largest / len(pieces))
        return jnp.repeat(jnp.exp(draws), dims[axis_at] // parts).reshape((-1,) + (1,) * (len(dims) - axis_at - 1))

    gain = one(*pieces[0])
    for cut in pieces[1:]:
        gain = gain * one(*cut)
    return gain


def normal_values(key, extent, scale, most, shards=(), held_as=jnp.bfloat16):
    values = scale * jax.random.normal(key, extent, jnp.float32)
    if shards:
        values = values * steps_of(key, extent, shards, -0.22, 0.18)
    return jnp.clip(values, -most, most).astype(held_as)


def setup_inputs(seed: int = 0) -> dict:
    key_list = jax.random.split(jax.random.key(seed), 13)
    return {
        "hop_feats": draw_hop_feats(jax.random.fold_in(key_list[12], 71), 0),
        "adj_local": normal_values(key_list[1], (NODES // TILE, KL, TILE, TILE), (TILE * (KL + KH)) ** -0.5, 0.125, ((0, 32),)),
        "local_cols": touch_ends(jax.random.randint(key_list[2], (NODES // TILE, KL), 0, RT), jax.random.fold_in(key_list[2], 1), 0, RT - 1).astype(jnp.int32),
        "adj_halo": normal_values(key_list[3], (NODES // TILE, KH, TILE, TILE), (TILE * (KL + KH)) ** -0.5, 0.125, ((0, 32),)),
        "halo_cols": touch_ends(jax.random.randint(key_list[4], (NODES // TILE, KH), 0, HALO_TILES), jax.random.fold_in(key_list[4], 1), 0, HALO_TILES - 1).astype(jnp.int32),
        "boundary_rows": touch_ends(jax.random.randint(key_list[5], (DEVICES, HALO_TILES * TILE), 0, RT * TILE), jax.random.fold_in(key_list[5], 1), 0, (RT * TILE) - 1).astype(jnp.int32),
        "train_ids": draw_train_ids(jax.random.fold_in(key_list[12], 71), 0),
        "shuffle": draw_shuffle(jax.random.fold_in(key_list[12], 71), 0),
        "labels": touch_ends(jax.random.randint(key_list[8], (NODES,), 0, CLASSES), jax.random.fold_in(key_list[8], 1), 0, CLASSES - 1).astype(jnp.int32),
        "labelled": draw_labelled(jax.random.fold_in(key_list[12], 71), 0),
        "w_first": draw_w_first(jax.random.fold_in(key_list[12], 71), 0),
        "w_second": draw_w_second(jax.random.fold_in(key_list[12], 71), 0),
    }


def loss_head(logits, targets, weights_row):
    row_max = lax.optimization_barrier(jnp.max(logits, axis=1, keepdims=True))
    expos = jnp.exp(logits - row_max)
    totals = lax.optimization_barrier(jnp.sum(expos, axis=1, keepdims=True))
    classes = lax.broadcasted_iota(jnp.int32, logits.shape, 1)
    onehot = (classes == targets[:, None]).astype(jnp.float32)
    cross = jnp.log(totals[:, 0]) + row_max[:, 0] - lax.optimization_barrier(jnp.sum(onehot * logits, axis=1))
    count = jnp.maximum(jnp.sum(weights_row), 1.0)
    dlogits = ((expos / totals - onehot) * (weights_row / count)[:, None]).astype(jnp.bfloat16)
    return (cross, dlogits)

def source_losses(cross, weights_row, groups):
    masks = weights_row.reshape(groups, -1)
    sums = lax.optimization_barrier(jnp.sum(masks * cross.reshape(groups, -1), axis=1))
    return sums / jnp.maximum(lax.optimization_barrier(jnp.sum(masks, axis=1)), 1.0)

def batch_norm(pre):
    center = pre - lax.optimization_barrier(jnp.mean(pre, axis=-2, keepdims=True))
    rstd = lax.rsqrt(lax.optimization_barrier(jnp.mean(center * center, axis=-2, keepdims=True)) + 1e-05)
    return (center * rstd, rstd)

def norm_back(grad, normed, rstd):
    mean_grad = lax.optimization_barrier(jnp.mean(grad, axis=-2, keepdims=True))
    mean_proj = lax.optimization_barrier(jnp.mean(grad * normed, axis=-2, keepdims=True))
    return (grad - mean_grad - normed * mean_proj) * rstd

def reference(hop_feats, adj_local, local_cols, adj_halo, halo_cols, boundary_rows, train_ids, shuffle, labels, labelled, w_first, w_second):
    devices = N_DOM * N_REP
    rows = RT * TILE
    share = HALO_TILES * TILE // devices
    hop_two = hop_feats[2]
    bases = jnp.arange(devices, dtype=jnp.int32)[:, None] * rows
    sources = (bases + boundary_rows).reshape(devices, devices, share)
    halo_ids = jnp.transpose(sources, (1, 0, 2)).reshape(devices, devices * share)
    loc_tiles = adj_local.reshape(devices, RT, KL, TILE, TILE)
    loc_cols = local_cols.reshape(devices, RT, KL)
    far_tiles = adj_halo.reshape(devices, RT, KH, TILE, TILE)
    far_cols = halo_cols.reshape(devices, RT, KH)

    def one_part(part):
        own = lax.dynamic_slice_in_dim(hop_two, part * rows, rows, 0)
        own = own.reshape(RT, TILE, D_FEAT).astype(jnp.float32)
        halo = hop_two[halo_ids[part]].reshape(HALO_TILES, TILE, D_FEAT).astype(jnp.float32)
        summed = jnp.einsum('ikab,ikbc->iac', loc_tiles[part].astype(jnp.float32), own[loc_cols[part]])
        summed = summed + jnp.einsum('ikab,ikbc->iac', far_tiles[part].astype(jnp.float32), halo[far_cols[part]])
        return summed.reshape(rows, D_FEAT).astype(jnp.bfloat16)
    next_hop = lax.map(one_part, jnp.arange(devices, dtype=jnp.int32)).reshape(devices * rows, D_FEAT)
    order = bases + jnp.take_along_axis(train_ids, shuffle, axis=1)
    per = SLOTS // devices
    batches = jnp.transpose(order.reshape(devices, devices, per), (1, 0, 2)).reshape(devices, SLOTS)
    allfeat = jnp.concatenate([hop_feats[0], hop_feats[1], hop_feats[2], next_hop], axis=1)

    def one_batch(carry, node_ids):
        grad_one, grad_two = carry
        inputs = allfeat[node_ids]
        targets = labels[node_ids]
        weights_row = labelled[node_ids].astype(jnp.float32)
        hidden_pre = jnp.dot(inputs, w_first, preferred_element_type=jnp.float32)
        normed, rstd = batch_norm(hidden_pre)
        hidden = jnp.maximum(normed, 0.0).astype(jnp.bfloat16)
        logits = jnp.dot(hidden, w_second, preferred_element_type=jnp.float32)
        cross, dlogits = loss_head(logits, targets, weights_row)
        loss = source_losses(cross, weights_row, devices)
        grad_two = grad_two + jnp.dot(hidden.T, dlogits, preferred_element_type=jnp.float32)
        dhidden = jnp.dot(dlogits, w_second.T, preferred_element_type=jnp.float32)
        masked = jnp.where(normed > 0, dhidden, 0.0)
        dpre = norm_back(masked, normed, rstd).astype(jnp.bfloat16)
        grad_one = grad_one + jnp.dot(inputs.T, dpre, preferred_element_type=jnp.float32)
        return ((grad_one, grad_two), loss)
    start = (jnp.zeros((4 * D_FEAT, HIDDEN_UNITS), jnp.float32), jnp.zeros((HIDDEN_UNITS, CLASSES), jnp.float32))
    (grad_first, grad_second), batch_loss = lax.scan(one_batch, start, batches)
    return (next_hop, batch_loss, grad_first, grad_second)
```

```python
import functools

import jax
import jax.numpy as jnp
from jax import lax
from jax.experimental import pallas as pl
from jax.experimental.pallas import tpu as pltpu
from jax.sharding import PartitionSpec as P

F32 = jnp.float32
BF16 = jnp.bfloat16
BIG = 60 * 1024 * 1024


def where_am_i(ndom, nrep):
    return lax.axis_index("dom") * nrep + lax.axis_index("rep")


def enter(me, n, nrep):
    barrier = pltpu.get_barrier_semaphore()

    def greet(o, carry):
        peer = lax.rem(me + o, n)
        pl.semaphore_signal(barrier, inc=1, device_id=(peer // nrep, lax.rem(peer, nrep)),
                            device_id_type=pl.DeviceIdType.MESH)
        return carry

    lax.fori_loop(1, n, greet, 0)
    pl.semaphore_wait(barrier, n - 1)


def spread(me, n, nrep, src_at, dst, send_sem, recv_sem):
    def copy(o):
        peer = lax.rem(me + o, n)
        return pltpu.make_async_remote_copy(
            src_ref=src_at(peer), dst_ref=dst.at[me],
            send_sem=send_sem.at[o], recv_sem=recv_sem.at[o],
            device_id=(peer // nrep, lax.rem(peer, nrep)),
            device_id_type=pl.DeviceIdType.MESH)

    def start(o, carry):
        copy(o).start()
        return carry

    def finish(o, carry):
        copy(o).wait()
        return carry

    return (lambda: lax.fori_loop(1, n, start, 0)), (lambda: lax.fori_loop(1, n, finish, 0))


def comm_call(kernel, outs, scratch, name, cid, *args):
    return pl.pallas_call(
        kernel,
        out_shape=outs,
        in_specs=[pl.BlockSpec(memory_space=pltpu.VMEM)] * len(args),
        out_specs=jax.tree.map(lambda _: pl.BlockSpec(memory_space=pltpu.VMEM), outs),
        scratch_shapes=scratch,
        compiler_params=pltpu.CompilerParams(collective_id=cid, has_side_effects=True),
        name=name,
    )(*args)


def dma_sems(n, count):
    return [pltpu.SemaphoreType.DMA((n,))] * count


def halo_kernel(ndom, nrep, src, cnt, out, tot, buf, crow, cbuf, ssem, rsem, s2, r2):
    n = ndom * nrep
    me = where_am_i(ndom, nrep)
    crow[0] = cnt[...]
    enter(me, n, nrep)
    start, finish = spread(me, n, nrep, lambda p: src.at[p], buf, ssem, rsem)
    cstart, cfinish = spread(me, n, nrep, lambda p: crow.at[0], cbuf, s2, r2)
    start()
    cstart()
    buf[me] = src[me]
    cbuf[me] = cnt[...]
    finish()
    cfinish()
    out[...] = buf[...]
    tot[...] = jnp.maximum(jnp.sum(cbuf[...], axis=0), 1.0)


def mlp_kernel(chunk, ndom, nrep, cores, classes, x3, tag, hop, w1, w2, counts, own_counts,
               first_out, second_out, loss_out,
               xs, xt, zs, gs, dzs, g2acc, acc, lrow, lbuf,
               fsrc, fin, fpart, fall, fgath, bsrc, bin_, bpart, ball, bgath,
               gsrc, gin, gsum, gnear, gfar, gkeep, gfarin,
               hsrc, hin, hsum, hnear, hkeep, hfar, hfarin, hgath,
               fx_s, fx_r, fa_s, fa_r, fg_s, fg_r, fw_s, fw_r,
               bx_s, bx_r, ba_s, ba_r, bg_s, bg_r, bw_s, bw_r,
               l_s, l_r, gx_s, gx_r, gn_s, gn_r, gf_s, gf_r,
               hx_s, hx_r, hn_s, hn_r, hf_s, hf_r, hg_s, hg_r):
    n = ndom * nrep
    chips = ndom // cores
    peers = chips * nrep
    dom, rep = lax.axis_index("dom"), lax.axis_index("rep")
    me = dom * nrep + rep
    chip, core = dom // cores, lax.rem(dom, cores)
    other = cores - 1 - core
    block = 256
    slots, hidden_units = zs.shape
    steps = slots // block
    groups = block // chunk
    half = fsrc.shape[1] // 2
    width = hidden_units // nrep
    per = half // nrep

    barrier = pltpu.get_barrier_semaphore()

    def greet(o, carry):
        peer = lax.rem(me + o, n)
        pl.semaphore_signal(barrier, inc=1, device_id=(peer // nrep, lax.rem(peer, nrep)),
                            device_id_type=pl.DeviceIdType.MESH)
        return carry

    lax.fori_loop(1, n, greet, 0)

    def to(src, dst, ssem, rsem, peer_dom, peer_rep):
        return pltpu.make_async_remote_copy(
            src_ref=src, dst_ref=dst, send_sem=ssem, recv_sem=rsem,
            device_id=(peer_dom, peer_rep), device_id_type=pl.DeviceIdType.MESH)

    def each(count, fn, first=0):
        lax.fori_loop(first, count, lambda i, carry: (fn(i), carry)[1], 0)

    def group_of(a, c):
        return pl.ds((a * cores + c) * nrep, nrep)

    def pre(i):
        at = pl.ds(pl.multiple_of(i * block, block), block)
        order = tag[at, 8:9].astype(jnp.int32)
        got = jnp.dot(one_hot(order, hop.shape[0]), hop[...], preferred_element_type=F32)
        x = jnp.concatenate([x3[at, :], got.astype(BF16)], axis=1)
        xs[at, :] = x
        here = pl.ds(i * groups, groups)
        for r in range(nrep):
            z = jnp.dot(x, w1[r], preferred_element_type=F32)
            zs[at, r * width:(r + 1) * width] = z
            z3 = z.reshape(groups, chunk, width)
            mean = jnp.sum(z3, axis=1, keepdims=True) * (1.0 / chunk)
            off = z3 - mean
            spread2 = jnp.sum(off * off, axis=1, keepdims=True)
            for j in range(per):
                cut = slice(j * 128, (j + 1) * 128)
                fsrc[here, r * per + j:r * per + j + 1] = mean[:, :, cut]
                fsrc[here, half + r * per + j:half + r * per + j + 1] = spread2[:, :, cut]

    each(steps, pre)
    pl.semaphore_wait(barrier, n - 1)

    def chip_sum(src, got, part, xs_, xr, combine):
        def swap(a):
            return to(src.at[group_of(a, other)], got.at[a], xs_.at[a], xr.at[a],
                      chip * cores + other, rep)

        def start():
            each(chips, lambda a: swap(a).start())

        def finish():
            def one(a):
                swap(a).wait()
                part[a] = combine(src[group_of(a, core)], got[a])
            each(chips, one)
        return start, finish

    def walk(o):
        return lax.rem(chip + o // nrep, chips), lax.rem(rep + lax.rem(o, nrep), nrep)

    def scatter(part, arrived, as_, ar):
        def copy(o):
            a, r = walk(o)
            return to(part.at[a, r], arrived.at[o], as_.at[o], ar.at[o], a * cores + core, r)

        def start():
            each(peers, lambda o: copy(o).start(), 1)
            arrived[0] = part[chip, rep]

        def finish():
            each(peers, lambda o: copy(o).wait(), 1)
        return start, finish

    def gather(gath, gs_, gr, ws, wr):
        def copy(o):
            a, r = walk(o)
            return to(gath.at[me], gath.at[me], gs_.at[o], gr.at[o], a * cores + core, r)

        def forward(da):
            at = group_of(lax.rem(chip + chips - da, chips), core)
            return to(gath.at[at], gath.at[at], ws.at[da], wr.at[da], chip * cores + other, rep)

        def start():
            each(peers, lambda o: copy(o).start(), 1)

        def finish():
            each(nrep, lambda o: copy(o).wait_recv(), 1)
            forward(0).start()

            def chip_in(da):
                each((da + 1) * nrep, lambda o: copy(o).wait_recv(), da * nrep)
                forward(da).start()
            each(chips, chip_in, 1)
            each(chips, lambda da: forward(da).wait())
            each(peers, lambda o: copy(o).wait_send(), 1)
        return start, finish

    def both_moments(a, b):
        ma, mb = a[:, :half], b[:, :half]
        gap = ma - mb
        spread2 = a[:, half:] + b[:, half:] + (0.5 * chunk) * gap * gap
        return jnp.concatenate([(ma + mb) * 0.5, spread2], axis=1)

    start, finish = chip_sum(fsrc, fin, fpart, fx_s, fx_r, both_moments)
    start()
    each(steps, lambda i: xt.__setitem__(
        (slice(None), pl.ds(pl.multiple_of(i * block, block), block)),
        xs[pl.ds(pl.multiple_of(i * block, block), block), :].T))
    finish()
    start, finish = scatter(fpart, fall, fa_s, fa_r)
    start()
    finish()
    got = fall[...]
    mu = jnp.sum(got[:, :half], axis=0) * (1.0 / peers)
    off = got[:, :half] - mu[None]
    m2 = jnp.sum(got[:, half:], axis=0) + (cores * chunk) * jnp.sum(off * off, axis=0)
    fgath[me] = jnp.concatenate([mu, lax.rsqrt(m2 * (1.0 / (n * chunk)) + 1e-05)], axis=0)
    start, finish = gather(fgath, fg_s, fg_r, fw_s, fw_r)
    start()
    g2acc[...] = jnp.zeros_like(g2acc)
    loss_row = jnp.zeros((1, lrow.shape[2]), F32)
    finish()

    second = w2[...]

    def head(i, loss_row):
        at = pl.ds(pl.multiple_of(i * block, block), block)
        here = pl.ds(i * groups, groups)
        z3 = zs[at, :].reshape(groups, chunk, hidden_units)
        st = fgath[here]
        mean = jnp.concatenate([st[:, j:j + 1] for j in range(half)], axis=2)
        rstd = jnp.concatenate([st[:, half + j:half + j + 1] for j in range(half)], axis=2)
        normed = ((z3 - mean) * rstd).reshape(block, hidden_units)
        zs[at, :] = normed
        hidden = jnp.maximum(normed, 0.0).astype(BF16)
        logits = jnp.dot(hidden, second, preferred_element_type=F32)
        lane = lax.broadcasted_iota(jnp.int32, logits.shape, 1)
        logits = jnp.where(lane < classes, logits, -1e30)
        row_max = jnp.max(logits, axis=1, keepdims=True)
        expos = jnp.exp(logits - row_max)
        totals = jnp.sum(expos, axis=1, keepdims=True)
        target = tag[at, 0:1].astype(jnp.int32)
        mark = tag[at, 1:2]
        onehot = (lane == target).astype(F32)
        cross = jnp.log(totals) + row_max - jnp.sum(onehot * logits, axis=1, keepdims=True)
        rows_at = i * block + lax.broadcasted_iota(jnp.int32, (block, counts.shape[1]), 0)
        mine = rows_at // chunk == lax.broadcasted_iota(jnp.int32, (block, counts.shape[1]), 1)
        count = jnp.sum(jnp.where(mine, counts[...], 0.0), axis=1, keepdims=True)
        dlogits = ((expos / totals - onehot) * (mark / count)).astype(BF16)
        g2acc[...] += lax.dot_general(hidden, dlogits, (((0,), (0,)), ((), ())), preferred_element_type=F32)
        masked = jnp.where(normed > 0, by_lanes(dlogits, second), 0.0)
        gs[at, :] = masked
        sums = jnp.sum(masked.reshape(groups, chunk, hidden_units), axis=1, keepdims=True)
        projs = jnp.sum((masked * normed).reshape(groups, chunk, hidden_units), axis=1, keepdims=True)
        for j in range(half):
            cut = slice(j * 128, (j + 1) * 128)
            bsrc[here, j:j + 1] = sums[:, :, cut]
            bsrc[here, half + j:half + j + 1] = projs[:, :, cut]
        return loss_row + jnp.sum(jnp.where(mine, mark * cross, 0.0), axis=0, keepdims=True)

    loss_row = lax.fori_loop(0, steps, head, loss_row)
    start, finish = chip_sum(bsrc, bin_, bpart, bx_s, bx_r, lambda a, b: a + b)
    start()
    loss_row = loss_row / jnp.maximum(own_counts[...], 1.0)
    lrow[0] = loss_row
    lbuf[me] = loss_row

    def send_loss(o):
        peer = lax.rem(me + o, n)
        return to(lrow.at[0], lbuf.at[me], l_s.at[o], l_r.at[o], peer // nrep, lax.rem(peer, nrep))

    part = hsrc.shape[3]
    for r in range(nrep):
        for d in range(ndom):
            first_row = (r * ndom + d) * part
            hsrc[d % cores, d // cores, r] = g2acc[first_row:first_row + part, :].astype(BF16)
    h_swap = to(hsrc.at[other], hin, hx_s.at[0], hx_r.at[0], chip * cores + other, rep)
    h_swap.start()
    finish()
    start, finish = scatter(bpart, ball, ba_s, ba_r)
    start()
    h_swap.wait()
    hsum[...] = (hsrc[core].astype(F32) + hin[...].astype(F32)).astype(BF16)
    finish()
    bgath[me] = jnp.sum(ball[...], axis=0) * (1.0 / (n * chunk))
    start, finish = gather(bgath, bg_s, bg_r, bw_s, bw_r)
    start()
    each(n, lambda o: send_loss(o).start(), 1)
    finish()

    def plane(o):
        return lax.rem(chip + o, chips)

    def h_near(o):
        return to(hsum.at[plane(o)], hnear.at[o - 1], hn_s.at[o], hn_r.at[o], plane(o) * cores + core, rep)

    def h_along(o):
        peer = lax.rem(rep + o, nrep)
        return to(hfar.at[peer], hfarin.at[o - 1], hf_s.at[o], hf_r.at[o], dom, peer)

    def h_round(o):
        return to(hgath.at[dom], hgath.at[dom], hg_s.at[o], hg_r.at[o], lax.rem(dom + o, ndom), rep)

    def h_stage(stage):
        if stage == 0:
            each(chips, lambda o: h_near(o).start(), 1)
        elif stage == 1:
            each(chips, lambda o: h_near(o).wait(), 1)
            total = hsrc[core, chip].astype(F32) + hin[chip].astype(F32)
            for o in range(1, chips):
                total = total + hnear[o - 1].astype(F32)
            hkeep[...] = total
            hfar[...] = total.astype(BF16)
            each(nrep, lambda o: h_along(o).start(), 1)
        elif stage == 2:
            each(nrep, lambda o: h_along(o).wait(), 1)
            total = hkeep[rep]
            for o in range(1, nrep):
                total = total + hfarin[o - 1].astype(F32)
            hgath[dom] = total
            each(ndom, lambda o: h_round(o).start(), 1)
        else:
            each(ndom, lambda o: h_round(o).wait(), 1)
            for d in range(ndom):
                second_out[d * part:(d + 1) * part, :] = hgath[d][:, :classes]

    high = acc.shape[0] // ndom

    def g_swap(r):
        return to(gsrc.at[r, other], gin.at[r], gx_s.at[r], gx_r.at[r], chip * cores + other, rep)

    def g_near(r, o):
        return to(gsum.at[r, plane(o)], gnear.at[r, o - 1], gn_s.at[r, o], gn_r.at[r, o],
                  plane(o) * cores + core, rep)

    def g_far(r):
        o = lax.rem(r - rep + nrep, nrep)
        return to(gfar.at[r], gfarin.at[o], gf_s.at[o], gf_r.at[o], dom, r)

    def g_stage(r, stage):
        if stage == 0:
            g_swap(r).start()
        elif stage == 1:
            g_swap(r).wait()
            gsum[r] = (gsrc[r, core].astype(F32) + gin[r].astype(F32)).astype(BF16)
            each(chips, lambda o: g_near(r, o).start(), 1)
        else:
            each(chips, lambda o: g_near(r, o).wait(), 1)
            total = gsrc[r, core, chip].astype(F32) + gin[r, chip].astype(F32)
            for o in range(1, chips):
                total = total + gnear[r, o - 1].astype(F32)
            gkeep[r] = total
            gfar[r] = total.astype(BF16)

            @pl.when(rep != r)
            def _():
                g_far(r).start()

    def tail(r):
        cols = slice(r * width, (r + 1) * width)

        def block_dz(i):
            at = pl.ds(pl.multiple_of(i * block, block), block)
            here = pl.ds(i * groups, groups)
            low = r * per

            def lines(ref, first):
                return jnp.concatenate(
                    [ref[here, first + j:first + j + 1] for j in range(per)], axis=2)

            masked = gs[at, cols].reshape(groups, chunk, width)
            normed = zs[at, cols].reshape(groups, chunk, width)
            dz = (masked - lines(bgath, low) - normed * lines(bgath, half + low)) * lines(fgath, half + low)
            dzs[at, :] = dz.reshape(block, width).astype(BF16)

        each(steps, block_dz)
        acc[...] = jnp.dot(xt[...], dzs[...], preferred_element_type=F32)
        for d in range(ndom):
            gsrc[r, d % cores, d // cores] = acc[d * high:(d + 1) * high, :].astype(BF16)

    for r in range(nrep):
        h_stage(r) if r < 4 else None
        tail(r)
        g_stage(r, 0)
        if r >= 1:
            g_stage(r - 1, 1)
        if r >= 2:
            g_stage(r - 2, 2)
    for s in range(nrep, 4):
        h_stage(s)
    g_stage(nrep - 1, 1)
    if nrep >= 2:
        g_stage(nrep - 2, 2)
    each(n, lambda o: send_loss(o).wait(), 1)
    losses = lbuf[...]
    source = lax.broadcasted_iota(jnp.int32, losses.shape, 0)
    lane = lax.broadcasted_iota(jnp.int32, losses.shape, 2)
    mine = jnp.sum(jnp.where(lane == me, losses, 0.0), axis=2, keepdims=True)
    loss_out[...] = jnp.sum(jnp.where(lane == source, mine, 0.0), axis=0)
    g_stage(nrep - 1, 2)

    def g_own(o):
        return to(gfar.at[rep], gfarin.at[o], gf_s.at[o], gf_r.at[o], dom, lax.rem(rep + o, nrep))

    each(nrep, lambda o: g_own(o).wait_recv(), 1)
    total = gkeep[rep]
    for o in range(1, nrep):
        total = total + gfarin[o].astype(F32)
    first_out[...] = total
    each(nrep, lambda o: g_own(o).wait_send(), 1)


def hop_kernel(kl, kh, lcols, hcols, adj_l, adj_h, own, halo, out):
    i = pl.program_id(0)
    left = jnp.concatenate([adj_l[0, k] for k in range(kl)] + [adj_h[0, k] for k in range(kh)], axis=1)
    right = jnp.concatenate(
        [own[0, lcols[i, k]] for k in range(kl)] + [halo[hcols[i, k]] for k in range(kh)], axis=0)
    out[0] = jnp.dot(left, right, preferred_element_type=F32).astype(BF16)


def batch_lanes(rows, wide, chunk):
    at = pl.program_id(0) * rows + lax.broadcasted_iota(jnp.int32, (rows, wide), 0)
    return at // chunk == lax.broadcasted_iota(jnp.int32, (rows, wide), 1)


def one_hot(column, count):
    lanes = lax.broadcasted_iota(jnp.int32, (column.shape[0], count), 1)
    return (lanes == column).astype(F32).astype(BF16)


def by_lanes(left, right):
    return lax.dot_general(left, right, (((1,), (1,)), ((), ())), preferred_element_type=F32)


def pick_kernel(chunk, shuf, bound, ids, labels, labelled, feats, x_out, tag_out, sent_out, cnt_out):
    rows = shuf.shape[0]
    nodes = feats.shape[1]
    sent_out[...] = jnp.dot(one_hot(bound[...], nodes), feats[2], preferred_element_type=F32).astype(BF16)
    numbers = ids[...]
    blank = jnp.zeros((6, nodes), F32)
    table = jnp.concatenate(
        [(numbers // 256).astype(F32), (numbers % 256).astype(F32), jnp.zeros((6, ids.shape[1]), F32)], axis=0)
    two = by_lanes(one_hot(shuf[...], ids.shape[1]), table.astype(BF16))
    order = two[:, 0:1] * 256.0 + two[:, 1:2]
    pick = one_hot(order.astype(jnp.int32), nodes)
    whole = jnp.concatenate([feats[0], feats[1], feats[2]], axis=1)
    x_out[...] = jnp.dot(pick, whole, preferred_element_type=F32).astype(BF16)
    marks = jnp.concatenate([labels[...].astype(F32), labelled[...].astype(F32), blank], axis=0)
    tags = by_lanes(pick, marks.astype(BF16))
    tag_out[:, 0:8] = tags
    tag_out[:, 8:9] = order

    @pl.when(pl.program_id(0) == 0)
    def _():
        cnt_out[...] = jnp.zeros_like(cnt_out)

    here = batch_lanes(rows, cnt_out.shape[1], chunk)
    cnt_out[...] += jnp.sum(jnp.where(here, tags[:, 1:2], 0.0), axis=0, keepdims=True)


def whole_spec(shape):
    return pl.BlockSpec(tuple(shape), lambda i: (0,) * len(shape))


def lead_spec(shape):
    return pl.BlockSpec(tuple(shape), lambda i: (i,) + (0,) * (len(shape) - 1))


def send_rep(half, nrep):
    return [lax.ppermute(half, "rep", [(s, (s + o) % nrep) for s in range(nrep)]) for o in range(1, nrep)]


def gather_rep(half, arrived, ndom, nrep, cores):
    dom, rep = lax.axis_index("dom"), lax.axis_index("rep")
    core = lax.rem(dom, cores)
    slots = jnp.zeros((nrep,) + half.shape, half.dtype)
    slots = lax.dynamic_update_slice(slots, half[None], (rep, 0, 0))
    for o in range(1, nrep):
        slots = lax.dynamic_update_slice(slots, arrived[o - 1][None], (lax.rem(rep - o + nrep, nrep), 0, 0))
    theirs = lax.ppermute(slots, "dom", [(d, d + 1 - 2 * (d % 2)) for d in range(ndom)])
    both = jnp.zeros((cores,) + slots.shape, slots.dtype)
    both = lax.dynamic_update_slice(both, slots[None], (core, 0, 0, 0))
    return lax.dynamic_update_slice(both, theirs[None], (cores - 1 - core, 0, 0, 0))


def shards(hop_feats, adj_local, local_cols, adj_halo, halo_cols, boundary_rows, train_ids,
           shuffle, labels, labelled, w_first, w_second):
    ndom, nrep = lax.axis_size("dom"), lax.axis_size("rep")
    n = ndom * nrep
    cores = 2
    row_tiles, kl, tile, _ = adj_local.shape
    kh = adj_halo.shape[1]
    rows, width = hop_feats.shape[1:]
    slots = train_ids.shape[1]
    hidden_units, classes = w_second.shape[0] * nrep, w_second.shape[1]
    chunk = slots // n
    block = 256
    steps = slots // block
    groups = block // chunk
    wide = -(-n // 128) * 128
    big = pltpu.CompilerParams(vmem_limit_bytes=BIG)
    sds = jax.ShapeDtypeStruct

    core = lax.rem(lax.axis_index("dom"), cores)
    own_cols = hidden_units // nrep
    h1, h2 = w_first.shape[0] // cores, w_second.shape[0] // cores
    half = jnp.concatenate([
        lax.dynamic_slice(w_first, (core * h1, 0), (h1, own_cols)),
        jnp.pad(lax.dynamic_slice(w_second, (core * h2, 0), (h2, classes)),
                ((0, 0), (0, own_cols - classes)))], axis=0)
    arrived = send_rep(half, nrep)

    sent_block = boundary_rows.shape[1] // steps
    x3, tags, sent, own_counts = pl.pallas_call(
        functools.partial(pick_kernel, chunk),
        out_shape=(sds((slots, 3 * width), BF16), sds((slots, 128), F32),
                   sds((boundary_rows.shape[1], width), BF16), sds((1, wide), F32)),
        grid=(steps,),
        in_specs=[lead_spec((block, 1)), lead_spec((sent_block, 1)), whole_spec((1, slots)),
                  whole_spec((1, rows)), whole_spec((1, rows)), whole_spec(hop_feats.shape)],
        out_specs=(lead_spec((block, 3 * width)), lead_spec((block, 128)),
                   lead_spec((sent_block, width)), whole_spec((1, wide))),
        compiler_params=big, name="pick",
        cost_estimate=pl.CostEstimate(flops=2 * slots * rows * 5 * width, bytes_accessed=4 << 20, transcendentals=0),
    )(shuffle[0][:, None], boundary_rows[0][:, None], train_ids, labels[None], labelled[None], hop_feats)

    arrived, own_counts = lax.optimization_barrier((arrived, own_counts))
    both = gather_rep(half, arrived, ndom, nrep, cores)
    sent = sent.reshape(n, -1, width)
    halo, counts = comm_call(
        functools.partial(halo_kernel, ndom, nrep), (sds(sent.shape, BF16), sds((1, wide), F32)),
        [pltpu.VMEM(sent.shape, BF16), pltpu.VMEM((1, 1, wide), F32), pltpu.VMEM((n, 1, wide), F32)]
        + dma_sems(n, 4), "halo", 1, sent, own_counts)
    halo = halo.reshape(-1, tile, width)

    next_hop = pl.pallas_call(
        functools.partial(hop_kernel, kl, kh),
        out_shape=sds((row_tiles, tile, width), BF16),
        grid=(row_tiles,),
        in_specs=[
            pl.BlockSpec(memory_space=pltpu.SMEM), pl.BlockSpec(memory_space=pltpu.SMEM),
            lead_spec((1, kl, tile, tile)), lead_spec((1, kh, tile, tile)),
            pl.BlockSpec((1, row_tiles, tile, width), lambda i: (2, 0, 0, 0)), whole_spec(halo.shape)],
        out_specs=lead_spec((1, tile, width)),
        compiler_params=big, name="hop",
        cost_estimate=pl.CostEstimate(flops=2 * rows * width * tile * (kl + kh), bytes_accessed=9 << 20, transcendentals=0),
    )(local_cols, halo_cols, adj_local, adj_halo, hop_feats.reshape(3, row_tiles, tile, width), halo)
    next_hop = next_hop.reshape(rows, width)

    w1 = both[:, :, :h1].transpose(1, 0, 2, 3).reshape(nrep, cores * h1, own_cols)
    w2 = both[:, :, h1:].transpose(1, 0, 2, 3).reshape(hidden_units, own_cols)
    span = own_cols

    lines = 2 * hidden_units // 128
    chips = ndom // cores
    peers = chips * nrep
    own_rows, part = 4 * width // ndom, hidden_units // n
    vm = pltpu.VMEM

    def moment_scratch():
        return [vm((n, lines, 128), F32), vm((chips, nrep, lines, 128), F32), vm((chips, nrep, lines, 128), F32),
                vm((peers, lines, 128), F32), vm((n, lines, 128), F32)]

    grad_block = (own_rows, own_cols)
    half_block = (part, span)
    scratch = [
        vm((slots, 4 * width), BF16), vm((4 * width, slots), BF16), vm((slots, hidden_units), F32),
        vm((slots, hidden_units), F32), vm((slots, own_cols), BF16), vm((hidden_units, span), F32),
        vm((4 * width, own_cols), F32), vm((1, 1, wide), F32), vm((n, 1, wide), F32),
        *moment_scratch(), *moment_scratch(),
        vm((nrep, cores, chips) + grad_block, BF16), vm((nrep, chips) + grad_block, BF16),
        vm((nrep, chips) + grad_block, BF16), vm((nrep, chips - 1) + grad_block, BF16),
        vm((nrep,) + grad_block, BF16), vm((nrep,) + grad_block, F32), vm((nrep,) + grad_block, BF16),
        vm((cores, chips, nrep) + half_block, BF16), vm((chips, nrep) + half_block, BF16),
        vm((chips, nrep) + half_block, BF16), vm((chips - 1, nrep) + half_block, BF16),
        vm((nrep,) + half_block, F32), vm((nrep,) + half_block, BF16), vm((nrep - 1,) + half_block, BF16),
        vm((ndom,) + half_block, F32),
    ]
    moment_sems = dma_sems(chips, 2) + dma_sems(peers, 4) + dma_sems(chips, 2)
    scratch += moment_sems + moment_sems + dma_sems(n, 2) + dma_sems(nrep, 2)
    scratch += [pltpu.SemaphoreType.DMA((nrep, chips))] * 2 + dma_sems(nrep, 2)
    scratch += dma_sems(1, 2) + dma_sems(chips, 2) + dma_sems(nrep, 2) + dma_sems(ndom, 2)
    vmem = pl.BlockSpec(memory_space=pltpu.VMEM)
    first, second, turned = pl.pallas_call(
        functools.partial(mlp_kernel, chunk, ndom, nrep, cores, classes),
        out_shape=(sds((own_rows, own_cols), F32), sds((hidden_units // nrep, classes), F32),
                   sds((1, wide), F32)),
        in_specs=[vmem] * 7,
        out_specs=(vmem, vmem, vmem),
        scratch_shapes=scratch,
        compiler_params=pltpu.CompilerParams(collective_id=2, has_side_effects=True, vmem_limit_bytes=BIG),
        name="mlp",
    )(x3, tags, next_hop, w1, w2, counts, own_counts)
    loss = turned[:, :n]
    return (next_hop, loss, first, second)


def solution(mesh):
    both = ("dom", "rep")
    placed = (
        P(None, both, None), P(both, None, None, None), P(both, None), P(both, None, None, None),
        P(both, None), P(both, None), P(both, None), P(both, None), P(both), P(both),
        P(None, "rep"), P("rep", None),
    )
    return jax.shard_map(
        shards, mesh=mesh, in_specs=placed,
        out_specs=(P(both, None), P(both, None), P("dom", "rep"), P("rep", None)),
        check_vma=False,
    )
```

```python
import functools

import jax
import jax.numpy as jnp
from jax import lax
from jax.experimental import pallas as pl
from jax.experimental.pallas import tpu as pltpu
from jax.sharding import PartitionSpec as P

F32 = jnp.float32
BF16 = jnp.bfloat16
BIG = 63 * 1024 * 1024
LANES = 128


def one_hot(column, count):
    lanes = lax.broadcasted_iota(jnp.int32, (column.shape[0], count), 1)
    return (lanes == column).astype(F32).astype(BF16)


def by_lanes(left, right):
    return lax.dot_general(left, right, (((1,), (1,)), ((), ())), preferred_element_type=F32)


def step_kernel(chunk, ndom, nrep, cores, classes, kl, kh,
               lcols, hcols, w1in, w2in, feats, adj_l, adj_h, tiles, bound, ids, shuf, labels, labelled,
               next_out, first_out, second_out, loss_out,
               ints, cols, order, whole, adjv, hacc, nh, pick, sent, halo, own_t, halo_t, tag, w1all, w2all, crow, cbuf,
               f_s, t_s, a_s, b_s, i_s, c_s, c_r, p_s, p_r, uz_s, uz_r, up_s, up_r, uc_s, uc_r,
               vz_s, vz_r, vp_s, vp_r, vc_s, vc_r,
               xs, xt, zs, gs, dzs, g2acc, acc, lrow, lbuf,
               fsrc, fin, fpart, fall, fgath, bsrc, bin_, bpart, ball, bgath,
               gsrc, gin, gsum, gnear, gfar, gkeep, gfarin,
               hsrc, hin, hsum, hnear, hkeep, hfar, hfarin, hgath,
               fx_s, fx_r, fa_s, fa_r, fg_s, fg_r, fw_s, fw_r,
               bx_s, bx_r, ba_s, ba_r, bg_s, bg_r, bw_s, bw_r,
               l_s, l_r, gx_s, gx_r, gn_s, gn_r, gf_s, gf_r,
               hx_s, hx_r, hn_s, hn_r, hf_s, hf_r, hg_s, hg_r):
    n = ndom * nrep
    chips = ndom // cores
    peers = chips * nrep
    dom, rep = lax.axis_index("dom"), lax.axis_index("rep")
    me = dom * nrep + rep
    chip, core = dom // cores, lax.rem(dom, cores)
    other = cores - 1 - core
    block = 256
    slots, hidden_units = zs.shape
    steps = slots // block
    groups = block // chunk
    half = fsrc.shape[1] // 2
    width = hidden_units // nrep
    per = half // nrep

    barrier = pltpu.get_barrier_semaphore()

    def greet(o, carry):
        peer = lax.rem(me + o, n)
        pl.semaphore_signal(barrier, inc=1, device_id=(peer // nrep, lax.rem(peer, nrep)),
                            device_id_type=pl.DeviceIdType.MESH)
        return carry

    lax.fori_loop(1, n, greet, 0)

    def to(src, dst, ssem, rsem, peer_dom, peer_rep):
        return pltpu.make_async_remote_copy(
            src_ref=src, dst_ref=dst, send_sem=ssem, recv_sem=rsem,
            device_id=(peer_dom, peer_rep), device_id_type=pl.DeviceIdType.MESH)

    def each(count, fn, first=0):
        lax.fori_loop(first, count, lambda i, carry: (fn(i), carry)[1], 0)

    def group_of(a, c):
        return pl.ds((a * cores + c) * nrep, nrep)

    def plane(o):
        return lax.rem(chip + o, chips)

    def rows_of(i):
        return pl.ds(pl.multiple_of(i * block, block), block)

    row_tiles, tile, fw = hacc.shape
    nodes = whole.shape[0]

    def feat_copy(k):
        return pltpu.make_async_copy(feats.at[k], whole.at[:, k * fw:(k + 1) * fw], f_s.at[k])

    def near_copy(i):
        return pltpu.make_async_copy(adj_l.at[i], adjv.at[i, 0:kl], a_s.at[i])

    def far_copy(i):
        return pltpu.make_async_copy(adj_h.at[i], adjv.at[i, kl:kl + kh], b_s.at[i])

    given = (shuf, ids, labels, labelled, bound)
    int_copies = [pltpu.make_async_copy(ref, ints.at[m:m + 1, 0:ref.shape[1]], i_s.at[m])
                  for m, ref in enumerate(given)]
    for copy in int_copies:
        copy.start()
    own_copy = pltpu.make_async_copy(tiles.at[2], own_t, t_s.at[0])
    own_copy.start()
    feat_copy(2).start()
    feat_copy(0).start()
    feat_copy(1).start()
    each(row_tiles, lambda i: near_copy(i).start())
    each(row_tiles, lambda i: far_copy(i).start())

    w1all[rep] = w1in[...].reshape(w1all.shape[1:])
    w2pad = jnp.concatenate(
        [w2in[...], jnp.zeros((w2in.shape[0], w2all.shape[3] - classes), BF16)], axis=1)
    w2all[rep] = w2pad.reshape(w2all.shape[1:])
    for copy in int_copies:
        copy.wait()

    def lines_of(m, count):
        return jnp.concatenate([ints[m:m + 1, j * LANES:(j + 1) * LANES] for j in range(count)], axis=0)

    per_slot, per_node, per_bound = slots // LANES, nodes // LANES, bound.shape[1] // LANES
    shuf_lines, id_lines = lines_of(0, per_slot), lines_of(1, per_slot)
    stack = [shuf_lines % LANES, shuf_lines // LANES, id_lines // LANES, id_lines % LANES,
             lines_of(2, per_node), lines_of(3, per_node), lines_of(4, per_bound)]
    used = sum(s.shape[0] for s in stack)
    stack = jnp.concatenate(stack + [jnp.zeros((LANES - used, LANES), jnp.int32)], axis=0)
    turned = stack.astype(F32).T
    cols[...] = turned

    def column(m):
        return cols[:, m:m + 1]

    at_bound = 2 * per_slot + 2 * per_slot + 2 * per_node
    own_copy.wait()
    last = own_t[...].reshape(nodes, fw)
    share = sent.shape[1]
    for m in range(per_bound):
        spot = one_hot(column(at_bound + m).astype(jnp.int32), nodes)
        rows = jnp.dot(spot, last, preferred_element_type=F32)
        count = LANES // share
        sent[m * count:(m + 1) * count] = rows.reshape(count, share, fw).astype(BF16)
    pl.semaphore_wait(barrier, n - 1)

    def send_halo(o):
        peer = lax.rem(me + o, n)
        return to(sent.at[peer], halo.at[me], p_s.at[o], p_r.at[o], peer // nrep, lax.rem(peer, nrep))

    def spread_weights(buf, zsem, zrec, psem, prec, csem, crec):
        def along(o):
            return to(buf.at[rep, dom], buf.at[rep, dom], zsem.at[o], zrec.at[o], dom, lax.rem(rep + o, nrep))

        def across(p, o):
            at = lax.rem(rep + o, nrep)
            return to(buf.at[at, dom], buf.at[at, dom], psem.at[p, o], prec.at[p, o],
                      plane(p) * cores + core, rep)

        def swap(p, o):
            at = lax.rem(rep + o, nrep)
            src = buf.at[at, lax.rem(chip - p + chips, chips) * cores + core]
            return to(src, src, csem.at[p, o], crec.at[p, o], chip * cores + other, rep)

        def each_pair(first, fn):
            each(chips, lambda p: each(nrep, lambda o: fn(p, o), 1), first)

        def stage(s):
            if s == 0:
                each(nrep, lambda o: along(o).start(), 1)
            elif s == 1:
                each(nrep, lambda o: along(o).wait(), 1)
                each_pair(1, lambda p, o: across(p, o).start())
                each(nrep, lambda o: swap(0, o).start(), 1)
            elif s == 2:
                each_pair(1, lambda p, o: across(p, o).wait())
                each_pair(1, lambda p, o: swap(p, o).start())
            else:
                each_pair(0, lambda p, o: swap(p, o).wait())
        return stage

    w1_stage = spread_weights(w1all, uz_s, uz_r, up_s, up_r, uc_s, uc_r)
    w2_stage = spread_weights(w2all, vz_s, vz_r, vp_s, vp_r, vc_s, vc_r)
    each(n, lambda o: send_halo(o).start(), 1)
    w1_stage(0)
    w2_stage(0)
    halo[me] = sent[me]

    lane = lax.broadcasted_iota(jnp.int32, (LANES, LANES), 1).astype(F32)
    table = cols[:, 2 * per_slot:4 * per_slot].astype(BF16)
    pair = lax.broadcasted_iota(jnp.int32, (LANES, 2 * per_slot), 1).astype(F32)
    for k in range(per_slot):
        low = (lane == column(k)).astype(F32).astype(BF16)
        found = jnp.dot(low, table, preferred_element_type=F32)
        high = column(per_slot + k)
        value = jnp.where(pair == high, found * LANES, jnp.where(pair == high + per_slot, found, 0.0))
        order[k * LANES:(k + 1) * LANES, 0:1] = jnp.sum(value, axis=1, keepdims=True)
    for k in range(per_node):
        marks = jnp.where(lane == 0, column(4 * per_slot + k),
                          jnp.where(lane == 1, column(4 * per_slot + per_node + k), 0.0))
        whole[k * LANES:(k + 1) * LANES, 3 * fw:4 * fw] = marks.astype(BF16)
    for k in range(3):
        feat_copy(k).wait()

    def batch_rows(i):
        rows_at = i * block + lax.broadcasted_iota(jnp.int32, (block, crow.shape[2]), 0)
        return rows_at // chunk == lax.broadcasted_iota(jnp.int32, (block, crow.shape[2]), 1)

    def gather_rows(i, own):
        at = rows_of(i)
        spot = one_hot(order[at, 0:1].astype(jnp.int32), nodes)
        pick[at, :] = spot
        rows = jnp.dot(spot, whole[...], preferred_element_type=F32)
        xs[at, 0:3 * fw] = rows[:, 0:3 * fw].astype(BF16)
        tags = rows[:, 3 * fw:4 * fw]
        tag[at, :] = tags
        return own + jnp.sum(jnp.where(batch_rows(i), tags[:, 1:2], 0.0), axis=0, keepdims=True)

    own_counts = lax.fori_loop(0, steps, gather_rows, jnp.zeros((1, crow.shape[2]), F32))
    w1_stage(1)
    w2_stage(1)
    crow[0] = own_counts
    cbuf[me] = own_counts

    def send_count(o):
        peer = lax.rem(me + o, n)
        return to(crow.at[0], cbuf.at[me], c_s.at[o], c_r.at[o], peer // nrep, lax.rem(peer, nrep))

    each(n, lambda o: send_count(o).start(), 1)

    def hop_near(i):
        near_copy(i).wait()
        left = jnp.concatenate([adjv[i, k] for k in range(kl)], axis=1)
        right = jnp.concatenate([own_t[lcols[i, k]] for k in range(kl)], axis=0)
        hacc[i] = jnp.dot(left, right, preferred_element_type=F32)

    each(row_tiles, hop_near)
    each(n, lambda o: send_halo(o).wait(), 1)
    halo_t[...] = halo[...].reshape(halo_t.shape)

    def hop_far(i):
        far_copy(i).wait()
        left = jnp.concatenate([adjv[i, kl + k] for k in range(kh)], axis=1)
        right = jnp.concatenate(
            [halo_t[hcols[i, k]] for k in range(kh)], axis=0)
        total = (hacc[i] + jnp.dot(left, right, preferred_element_type=F32)).astype(BF16)
        nh[pl.ds(pl.multiple_of(i * tile, tile), tile), :] = total
        next_out[pl.ds(pl.multiple_of(i * tile, tile), tile), :] = total

    each(row_tiles, hop_far)
    w1_stage(2)
    w2_stage(2)

    def gather_next(i):
        at = rows_of(i)
        xs[at, 3 * fw:4 * fw] = jnp.dot(pick[at, :], nh[...], preferred_element_type=F32).astype(BF16)

    each(steps, gather_next)
    w1_stage(3)

    def pre(i):
        at = rows_of(i)
        here = pl.ds(i * groups, groups)
        x = xs[at, :]
        for r in range(nrep):
            w1 = w1all[r].reshape(w1in.shape)
            z = jnp.dot(x, w1, preferred_element_type=F32)
            zs[at, r * width:(r + 1) * width] = z
            z3 = z.reshape(groups, chunk, width)
            mean = jnp.sum(z3, axis=1, keepdims=True) * (1.0 / chunk)
            off = z3 - mean
            spread2 = jnp.sum(off * off, axis=1, keepdims=True)
            for j in range(per):
                cut = slice(j * 128, (j + 1) * 128)
                fsrc[here, r * per + j:r * per + j + 1] = mean[:, :, cut]
                fsrc[here, half + r * per + j:half + r * per + j + 1] = spread2[:, :, cut]

    each(steps, pre)

    def chip_sum(src, got, part, xs_, xr, combine):
        def swap(a):
            return to(src.at[group_of(a, other)], got.at[a], xs_.at[a], xr.at[a],
                      chip * cores + other, rep)

        def start():
            each(chips, lambda a: swap(a).start())

        def finish():
            def one(a):
                swap(a).wait()
                part[a] = combine(src[group_of(a, core)], got[a])
            each(chips, one)
        return start, finish

    def walk(o):
        return lax.rem(chip + o // nrep, chips), lax.rem(rep + lax.rem(o, nrep), nrep)

    def scatter(part, arrived, as_, ar):
        def copy(o):
            a, r = walk(o)
            return to(part.at[a, r], arrived.at[o], as_.at[o], ar.at[o], a * cores + core, r)

        def start():
            each(peers, lambda o: copy(o).start(), 1)
            arrived[0] = part[chip, rep]

        def finish():
            each(peers, lambda o: copy(o).wait(), 1)
        return start, finish

    def gather(gath, gs_, gr, ws, wr):
        def copy(o):
            a, r = walk(o)
            return to(gath.at[me], gath.at[me], gs_.at[o], gr.at[o], a * cores + core, r)

        def forward(da):
            at = group_of(lax.rem(chip + chips - da, chips), core)
            return to(gath.at[at], gath.at[at], ws.at[da], wr.at[da], chip * cores + other, rep)

        def start():
            each(peers, lambda o: copy(o).start(), 1)

        def finish():
            each(nrep, lambda o: copy(o).wait_recv(), 1)
            forward(0).start()

            def chip_in(da):
                each((da + 1) * nrep, lambda o: copy(o).wait_recv(), da * nrep)
                forward(da).start()
            each(chips, chip_in, 1)
            each(chips, lambda da: forward(da).wait())
            each(peers, lambda o: copy(o).wait_send(), 1)
        return start, finish

    def both_moments(a, b):
        ma, mb = a[:, :half], b[:, :half]
        gap = ma - mb
        spread2 = a[:, half:] + b[:, half:] + (0.5 * chunk) * gap * gap
        return jnp.concatenate([(ma + mb) * 0.5, spread2], axis=1)

    start, finish = chip_sum(fsrc, fin, fpart, fx_s, fx_r, both_moments)
    start()
    each(steps, lambda i: xt.__setitem__(
        (slice(None), pl.ds(pl.multiple_of(i * block, block), block)),
        xs[pl.ds(pl.multiple_of(i * block, block), block), :].T))
    finish()
    start, finish = scatter(fpart, fall, fa_s, fa_r)
    start()
    finish()
    got = fall[...]
    mu = jnp.sum(got[:, :half], axis=0) * (1.0 / peers)
    off = got[:, :half] - mu[None]
    m2 = jnp.sum(got[:, half:], axis=0) + (cores * chunk) * jnp.sum(off * off, axis=0)
    fgath[me] = jnp.concatenate([mu, lax.rsqrt(m2 * (1.0 / (n * chunk)) + 1e-05)], axis=0)
    start, finish = gather(fgath, fg_s, fg_r, fw_s, fw_r)
    start()
    g2acc[...] = jnp.zeros_like(g2acc)
    loss_row = jnp.zeros((1, lrow.shape[2]), F32)
    w2_stage(3)
    each(n, lambda o: send_count(o).wait(), 1)
    counts = jnp.maximum(jnp.sum(cbuf[...], axis=0), 1.0)
    finish()

    second = w2all[...].reshape(hidden_units, w2all.shape[3])

    def head(i, loss_row):
        at = pl.ds(pl.multiple_of(i * block, block), block)
        here = pl.ds(i * groups, groups)
        z3 = zs[at, :].reshape(groups, chunk, hidden_units)
        st = fgath[here]
        mean = jnp.concatenate([st[:, j:j + 1] for j in range(half)], axis=2)
        rstd = jnp.concatenate([st[:, half + j:half + j + 1] for j in range(half)], axis=2)
        normed = ((z3 - mean) * rstd).reshape(block, hidden_units)
        zs[at, :] = normed
        hidden = jnp.maximum(normed, 0.0).astype(BF16)
        logits = jnp.dot(hidden, second, preferred_element_type=F32)
        lane = lax.broadcasted_iota(jnp.int32, logits.shape, 1)
        logits = jnp.where(lane < classes, logits, -1e30)
        row_max = jnp.max(logits, axis=1, keepdims=True)
        expos = jnp.exp(logits - row_max)
        totals = jnp.sum(expos, axis=1, keepdims=True)
        target = tag[at, 0:1].astype(jnp.int32)
        mark = tag[at, 1:2]
        onehot = (lane == target).astype(F32)
        cross = jnp.log(totals) + row_max - jnp.sum(onehot * logits, axis=1, keepdims=True)
        mine = batch_rows(i)
        count = jnp.sum(jnp.where(mine, counts, 0.0), axis=1, keepdims=True)
        dlogits = ((expos / totals - onehot) * (mark / count)).astype(BF16)
        g2acc[...] += lax.dot_general(hidden, dlogits, (((0,), (0,)), ((), ())), preferred_element_type=F32)
        masked = jnp.where(normed > 0, by_lanes(dlogits, second), 0.0)
        gs[at, :] = masked
        sums = jnp.sum(masked.reshape(groups, chunk, hidden_units), axis=1, keepdims=True)
        projs = jnp.sum((masked * normed).reshape(groups, chunk, hidden_units), axis=1, keepdims=True)
        for j in range(half):
            cut = slice(j * 128, (j + 1) * 128)
            bsrc[here, j:j + 1] = sums[:, :, cut]
            bsrc[here, half + j:half + j + 1] = projs[:, :, cut]
        return loss_row + jnp.sum(jnp.where(mine, mark * cross, 0.0), axis=0, keepdims=True)

    loss_row = lax.fori_loop(0, steps, head, loss_row)
    start, finish = chip_sum(bsrc, bin_, bpart, bx_s, bx_r, lambda a, b: a + b)
    start()
    loss_row = loss_row / jnp.maximum(own_counts, 1.0)
    lrow[0] = loss_row
    lbuf[me] = loss_row

    def send_loss(o):
        peer = lax.rem(me + o, n)
        return to(lrow.at[0], lbuf.at[me], l_s.at[o], l_r.at[o], peer // nrep, lax.rem(peer, nrep))

    part = hsrc.shape[3]
    for r in range(nrep):
        for d in range(ndom):
            first_row = (r * ndom + d) * part
            hsrc[d % cores, d // cores, r] = g2acc[first_row:first_row + part, :].astype(BF16)
    h_swap = to(hsrc.at[other], hin, hx_s.at[0], hx_r.at[0], chip * cores + other, rep)
    h_swap.start()
    finish()
    start, finish = scatter(bpart, ball, ba_s, ba_r)
    start()
    h_swap.wait()
    hsum[...] = (hsrc[core].astype(F32) + hin[...].astype(F32)).astype(BF16)
    finish()
    bgath[me] = jnp.sum(ball[...], axis=0) * (1.0 / (n * chunk))
    start, finish = gather(bgath, bg_s, bg_r, bw_s, bw_r)
    start()
    each(n, lambda o: send_loss(o).start(), 1)
    finish()

    def h_near(o):
        return to(hsum.at[plane(o)], hnear.at[o - 1], hn_s.at[o], hn_r.at[o], plane(o) * cores + core, rep)

    def h_along(o):
        peer = lax.rem(rep + o, nrep)
        return to(hfar.at[peer], hfarin.at[o - 1], hf_s.at[o], hf_r.at[o], dom, peer)

    def h_round(o):
        return to(hgath.at[dom], hgath.at[dom], hg_s.at[o], hg_r.at[o], lax.rem(dom + o, ndom), rep)

    def h_stage(stage):
        if stage == 0:
            each(chips, lambda o: h_near(o).start(), 1)
        elif stage == 1:
            each(chips, lambda o: h_near(o).wait(), 1)
            total = hsrc[core, chip].astype(F32) + hin[chip].astype(F32)
            for o in range(1, chips):
                total = total + hnear[o - 1].astype(F32)
            hkeep[...] = total
            hfar[...] = total.astype(BF16)
            each(nrep, lambda o: h_along(o).start(), 1)
        elif stage == 2:
            each(nrep, lambda o: h_along(o).wait(), 1)
            total = hkeep[rep]
            for o in range(1, nrep):
                total = total + hfarin[o - 1].astype(F32)
            hgath[dom] = total
            each(ndom, lambda o: h_round(o).start(), 1)
        else:
            each(ndom, lambda o: h_round(o).wait(), 1)
            for d in range(ndom):
                second_out[d * part:(d + 1) * part, :] = hgath[d][:, :classes]

    high = acc.shape[0] // ndom

    def g_swap(r):
        return to(gsrc.at[r, other], gin.at[r], gx_s.at[r], gx_r.at[r], chip * cores + other, rep)

    def g_near(r, o):
        return to(gsum.at[r, plane(o)], gnear.at[r, o - 1], gn_s.at[r, o], gn_r.at[r, o],
                  plane(o) * cores + core, rep)

    def g_far(r):
        o = lax.rem(r - rep + nrep, nrep)
        return to(gfar.at[r], gfarin.at[o], gf_s.at[o], gf_r.at[o], dom, r)

    def g_stage(r, stage):
        if stage == 0:
            g_swap(r).start()
        elif stage == 1:
            g_swap(r).wait()
            gsum[r] = (gsrc[r, core].astype(F32) + gin[r].astype(F32)).astype(BF16)
            each(chips, lambda o: g_near(r, o).start(), 1)
        else:
            each(chips, lambda o: g_near(r, o).wait(), 1)
            total = gsrc[r, core, chip].astype(F32) + gin[r, chip].astype(F32)
            for o in range(1, chips):
                total = total + gnear[r, o - 1].astype(F32)
            gkeep[r] = total
            gfar[r] = total.astype(BF16)

            @pl.when(rep != r)
            def _():
                g_far(r).start()

    def tail(r):
        cols = slice(r * width, (r + 1) * width)

        def block_dz(i):
            at = pl.ds(pl.multiple_of(i * block, block), block)
            here = pl.ds(i * groups, groups)
            low = r * per

            def lines(ref, first):
                return jnp.concatenate(
                    [ref[here, first + j:first + j + 1] for j in range(per)], axis=2)

            masked = gs[at, cols].reshape(groups, chunk, width)
            normed = zs[at, cols].reshape(groups, chunk, width)
            dz = (masked - lines(bgath, low) - normed * lines(bgath, half + low)) * lines(fgath, half + low)
            dzs[at, :] = dz.reshape(block, width).astype(BF16)

        each(steps, block_dz)
        acc[...] = jnp.dot(xt[...], dzs[...], preferred_element_type=F32)
        for d in range(ndom):
            gsrc[r, d % cores, d // cores] = acc[d * high:(d + 1) * high, :].astype(BF16)

    for r in range(nrep):
        h_stage(r) if r < 4 else None
        tail(r)
        g_stage(r, 0)
        if r >= 1:
            g_stage(r - 1, 1)
        if r >= 2:
            g_stage(r - 2, 2)
    for s in range(nrep, 4):
        h_stage(s)
    g_stage(nrep - 1, 1)
    if nrep >= 2:
        g_stage(nrep - 2, 2)
    each(n, lambda o: send_loss(o).wait(), 1)
    losses = lbuf[...]
    source = lax.broadcasted_iota(jnp.int32, losses.shape, 0)
    lane = lax.broadcasted_iota(jnp.int32, losses.shape, 2)
    mine = jnp.sum(jnp.where(lane == me, losses, 0.0), axis=2, keepdims=True)
    loss_out[...] = jnp.sum(jnp.where(lane == source, mine, 0.0), axis=0)[:, :n]
    g_stage(nrep - 1, 2)

    def g_own(o):
        return to(gfar.at[rep], gfarin.at[o], gf_s.at[o], gf_r.at[o], dom, lax.rem(rep + o, nrep))

    each(nrep, lambda o: g_own(o).wait_recv(), 1)
    total = gkeep[rep]
    for o in range(1, nrep):
        total = total + gfarin[o].astype(F32)
    first_out[...] = total
    each(nrep, lambda o: g_own(o).wait_send(), 1)


def hop_kernel(kl, kh, lcols, hcols, adj_l, adj_h, own, halo, out):
    i = pl.program_id(0)
    left = jnp.concatenate([adj_l[0, k] for k in range(kl)] + [adj_h[0, k] for k in range(kh)], axis=1)
    right = jnp.concatenate(
        [own[0, lcols[i, k]] for k in range(kl)] + [halo[hcols[i, k]] for k in range(kh)], axis=0)
    out[0] = jnp.dot(left, right, preferred_element_type=F32).astype(BF16)


def batch_lanes(rows, wide, chunk):
    at = pl.program_id(0) * rows + lax.broadcasted_iota(jnp.int32, (rows, wide), 0)
    return at // chunk == lax.broadcasted_iota(jnp.int32, (rows, wide), 1)


def one_hot(column, count):
    lanes = lax.broadcasted_iota(jnp.int32, (column.shape[0], count), 1)
    return (lanes == column).astype(F32).astype(BF16)


def by_lanes(left, right):
    return lax.dot_general(left, right, (((1,), (1,)), ((), ())), preferred_element_type=F32)


def pick_kernel(chunk, shuf, bound, ids, labels, labelled, feats, x_out, tag_out, sent_out, cnt_out):
    rows = shuf.shape[0]
    nodes = feats.shape[1]
    sent_out[...] = jnp.dot(one_hot(bound[...], nodes), feats[2], preferred_element_type=F32).astype(BF16)
    numbers = ids[...]
    blank = jnp.zeros((6, nodes), F32)
    table = jnp.concatenate(
        [(numbers // 256).astype(F32), (numbers % 256).astype(F32), jnp.zeros((6, ids.shape[1]), F32)], axis=0)
    two = by_lanes(one_hot(shuf[...], ids.shape[1]), table.astype(BF16))
    order = two[:, 0:1] * 256.0 + two[:, 1:2]
    pick = one_hot(order.astype(jnp.int32), nodes)
    whole = jnp.concatenate([feats[0], feats[1], feats[2]], axis=1)
    x_out[...] = jnp.dot(pick, whole, preferred_element_type=F32).astype(BF16)
    marks = jnp.concatenate([labels[...].astype(F32), labelled[...].astype(F32), blank], axis=0)
    tags = by_lanes(pick, marks.astype(BF16))
    tag_out[:, 0:8] = tags
    tag_out[:, 8:9] = order

    @pl.when(pl.program_id(0) == 0)
    def _():
        cnt_out[...] = jnp.zeros_like(cnt_out)

    here = batch_lanes(rows, cnt_out.shape[1], chunk)
    cnt_out[...] += jnp.sum(jnp.where(here, tags[:, 1:2], 0.0), axis=0, keepdims=True)


def dma_sems(n, count):
    return [pltpu.SemaphoreType.DMA((n,))] * count


def shards(hop_feats, adj_local, local_cols, adj_halo, halo_cols, boundary_rows, train_ids,
           shuffle, labels, labelled, w_first, w_second):
    ndom, nrep = lax.axis_size("dom"), lax.axis_size("rep")
    n = ndom * nrep
    cores = 2
    row_tiles, kl, tile, _ = adj_local.shape
    kh = adj_halo.shape[1]
    nodes, width = hop_feats.shape[1:]
    slots = train_ids.shape[1]
    hidden_units, classes = w_second.shape[0] * nrep, w_second.shape[1]
    chunk = slots // n
    wide = -(-n // LANES) * LANES
    sds = jax.ShapeDtypeStruct
    own_cols = hidden_units // nrep
    span = -(-classes // LANES) * LANES
    lines = 2 * hidden_units // LANES
    chips = ndom // cores
    peers = chips * nrep
    own_rows, part = 4 * width // ndom, hidden_units // n
    share = boundary_rows.shape[1] // n
    vm = pltpu.VMEM

    def moment_scratch():
        return [vm((n, lines, LANES), F32), vm((chips, nrep, lines, LANES), F32),
                vm((chips, nrep, lines, LANES), F32), vm((peers, lines, LANES), F32), vm((n, lines, LANES), F32)]

    def pairs(a, b, count):
        return [pltpu.SemaphoreType.DMA((a, b))] * count

    grad_block = (own_rows, own_cols)
    half_block = (part, span)
    scratch = [
        vm((8, max(slots, nodes)), jnp.int32), vm((LANES, LANES), F32), vm((slots, LANES), F32),
        vm((nodes, 4 * width), BF16), vm((row_tiles, kl + kh, tile, tile), BF16),
        vm((row_tiles, tile, width), F32), vm((nodes, width), BF16), vm((slots, nodes), BF16),
        vm((n, share, width), BF16), vm((n, share, width), BF16), vm((row_tiles, tile, width), BF16),
        vm((n * share // tile, tile, width), BF16), vm((slots, width), F32),
        vm((nrep, ndom, 4 * width // ndom, own_cols), BF16),
        vm((nrep, ndom, own_cols // ndom, span), BF16),
        vm((1, 1, wide), F32), vm((n, 1, wide), F32),
    ]
    scratch += dma_sems(3, 1) + dma_sems(1, 1) + dma_sems(row_tiles, 2) + dma_sems(5, 1) + dma_sems(n, 4)
    weight_sems = dma_sems(nrep, 2) + pairs(chips, nrep, 4)
    scratch += weight_sems + weight_sems
    scratch += [
        vm((slots, 4 * width), BF16), vm((4 * width, slots), BF16), vm((slots, hidden_units), F32),
        vm((slots, hidden_units), F32), vm((slots, own_cols), BF16), vm((hidden_units, span), F32),
        vm((4 * width, own_cols), F32), vm((1, 1, wide), F32), vm((n, 1, wide), F32),
        *moment_scratch(), *moment_scratch(),
        vm((nrep, cores, chips) + grad_block, BF16), vm((nrep, chips) + grad_block, BF16),
        vm((nrep, chips) + grad_block, BF16), vm((nrep, chips - 1) + grad_block, BF16),
        vm((nrep,) + grad_block, BF16), vm((nrep,) + grad_block, F32), vm((nrep,) + grad_block, BF16),
        vm((cores, chips, nrep) + half_block, BF16), vm((chips, nrep) + half_block, BF16),
        vm((chips, nrep) + half_block, BF16), vm((chips - 1, nrep) + half_block, BF16),
        vm((nrep,) + half_block, F32), vm((nrep,) + half_block, BF16), vm((nrep - 1,) + half_block, BF16),
        vm((ndom,) + half_block, F32),
    ]
    moment_sems = dma_sems(chips, 2) + dma_sems(peers, 4) + dma_sems(chips, 2)
    scratch += moment_sems + moment_sems + dma_sems(n, 2) + dma_sems(nrep, 2)
    scratch += pairs(nrep, chips, 2) + dma_sems(nrep, 2)
    scratch += dma_sems(1, 2) + dma_sems(chips, 2) + dma_sems(nrep, 2) + dma_sems(ndom, 2)
    vmem = pl.BlockSpec(memory_space=pltpu.VMEM)
    smem = pl.BlockSpec(memory_space=pltpu.SMEM)
    where = pl.BlockSpec(memory_space=pl.ANY)
    next_hop, first, second, loss = pl.pallas_call(
        functools.partial(step_kernel, chunk, ndom, nrep, cores, classes, kl, kh),
        out_shape=(sds((nodes, width), BF16), sds((own_rows, own_cols), F32),
                   sds((hidden_units // nrep, classes), F32), sds((1, n), F32)),
        in_specs=[smem, smem, vmem, vmem] + [where] * 9,
        out_specs=(vmem, vmem, vmem, vmem),
        scratch_shapes=scratch,
        compiler_params=pltpu.CompilerParams(collective_id=2, has_side_effects=True, vmem_limit_bytes=BIG),
        name="step",
    )(local_cols, halo_cols, w_first, w_second, hop_feats, adj_local, adj_halo,
      hop_feats.reshape(3, row_tiles, tile, width), boundary_rows,
      train_ids, shuffle, labels[None], labelled[None])
    return (next_hop, loss, first, second)


def solution(mesh):
    both = ("dom", "rep")
    placed = (
        P(None, both, None), P(both, None, None, None), P(both, None), P(both, None, None, None),
        P(both, None), P(both, None), P(both, None), P(both, None), P(both), P(both),
        P(None, "rep"), P("rep", None),
    )
    return jax.shard_map(
        shards, mesh=mesh, in_specs=placed,
        out_specs=(P(both, None), P(both, None), P("dom", "rep"), P("rep", None)),
        check_vma=False,
    )
```

```python
import functools

import jax
import jax.numpy as jnp
from jax import lax
from jax.experimental import pallas as pl
from jax.experimental.pallas import tpu as pltpu
from jax.sharding import PartitionSpec as P

F32 = jnp.float32
BF16 = jnp.bfloat16
BIG = 63 * 1024 * 1024
LANES = 128


def one_hot(column, count):
    lanes = lax.broadcasted_iota(jnp.int32, (column.shape[0], count), 1)
    return (lanes == column).astype(F32).astype(BF16)


def by_lanes(left, right):
    return lax.dot_general(left, right, (((1,), (1,)), ((), ())), preferred_element_type=F32)


def step_kernel(chunk, ndom, nrep, cores, classes, kl, kh,
               lcols, hcols, w1in, w2in, feats, adj_l, adj_h, tiles, bound, ids, shuf, labels, labelled,
               next_out, first_out, second_out, loss_out,
               ints, cols, order, whole, adjv, hacc, nh, pick, sent, halo, own_t, halo_t, tag, w1all, w2all, w2t, crow, cbuf,
               f_s, t_s, a_s, b_s, i_s, c_s, c_r, p_s, p_r, u_s, v_s,
               xs, xt, zs, gs, dzs, g2acc, acc, lrow, lbuf,
               fsrc, fin, fpart, fall, fgath, bsrc, bin_, bpart, ball, bgath,
               gsrc, gin, gsum, gnear, gfar, gkeep, gfarin,
               hsrc, hin, hsum, hnear, hkeep, hfar, hfarin, hgath,
               fx_s, fx_r, fa_s, fa_r, fg_s, fg_r, fw_s, fw_r,
               bx_s, bx_r, ba_s, ba_r, bg_s, bg_r, bw_s, bw_r,
               l_s, l_r, gx_s, gx_r, gn_s, gn_r, gf_s, gf_r,
               hx_s, hx_r, hn_s, hn_r, hf_s, hf_r, hg_s, hg_r):
    n = ndom * nrep
    chips = ndom // cores
    peers = chips * nrep
    dom, rep = lax.axis_index("dom"), lax.axis_index("rep")
    me = dom * nrep + rep
    chip, core = dom // cores, lax.rem(dom, cores)
    other = cores - 1 - core
    block = 256
    slots, hidden_units = zs.shape
    steps = slots // block
    groups = block // chunk
    half = fsrc.shape[1] // 2
    width = hidden_units // nrep
    per = half // nrep

    barrier = pltpu.get_barrier_semaphore()

    def greet(o, carry):
        peer = lax.rem(me + o, n)
        pl.semaphore_signal(barrier, inc=1, device_id=(peer // nrep, lax.rem(peer, nrep)),
                            device_id_type=pl.DeviceIdType.MESH)
        return carry

    lax.fori_loop(1, n, greet, 0)

    def to(src, dst, ssem, rsem, peer_dom, peer_rep):
        return pltpu.make_async_remote_copy(
            src_ref=src, dst_ref=dst, send_sem=ssem, recv_sem=rsem,
            device_id=(peer_dom, peer_rep), device_id_type=pl.DeviceIdType.MESH)

    def each(count, fn, first=0):
        lax.fori_loop(first, count, lambda i, carry: (fn(i), carry)[1], 0)

    def group_of(a, c):
        return pl.ds((a * cores + c) * nrep, nrep)

    def plane(o):
        return lax.rem(chip + o, chips)

    def rows_of(i):
        return pl.ds(pl.multiple_of(i * block, block), block)

    row_tiles, tile, fw = hacc.shape
    nodes = whole.shape[0]

    def feat_copy(k):
        return pltpu.make_async_copy(feats.at[k], whole.at[:, k * fw:(k + 1) * fw], f_s.at[k])

    bands = a_s.shape[0]
    deep = row_tiles // bands

    def near_copy(j):
        at = pl.ds(j * deep, deep)
        return pltpu.make_async_copy(adj_l.at[at], adjv.at[at, 0:kl], a_s.at[j])

    def far_copy(j):
        at = pl.ds(j * deep, deep)
        return pltpu.make_async_copy(adj_h.at[at], adjv.at[at, kl:kl + kh], b_s.at[j])

    given = (shuf, ids, labels, labelled, bound)
    int_copies = [pltpu.make_async_copy(ref, ints.at[m:m + 1, 0:ref.shape[1]], i_s.at[m])
                  for m, ref in enumerate(given)]
    for copy in int_copies:
        copy.start()
    own_copy = pltpu.make_async_copy(tiles.at[2], own_t, t_s.at[0])
    own_copy.start()
    feat_copy(2).start()
    feat_copy(0).start()
    feat_copy(1).start()
    each(bands, lambda j: near_copy(j).start())
    each(bands, lambda j: far_copy(j).start())

    w1all[rep] = w1in[...].reshape(w1all.shape[1:])
    w2t[...] = jnp.zeros_like(w2t)
    w2t[0:classes, :] = w2in[...].astype(F32)
    w2all[rep] = w2t[...].T.astype(BF16).reshape(w2all.shape[1:])
    for copy in int_copies:
        copy.wait()

    def lines_of(m, count):
        return jnp.concatenate([ints[m:m + 1, j * LANES:(j + 1) * LANES] for j in range(count)], axis=0)

    per_slot, per_node, per_bound = slots // LANES, nodes // LANES, bound.shape[1] // LANES
    shuf_lines, id_lines = lines_of(0, per_slot), lines_of(1, per_slot)
    stack = [shuf_lines % LANES, shuf_lines // LANES, id_lines // LANES, id_lines % LANES,
             lines_of(2, per_node), lines_of(3, per_node), lines_of(4, per_bound)]
    used = sum(s.shape[0] for s in stack)
    stack = jnp.concatenate(stack + [jnp.zeros((LANES - used, LANES), jnp.int32)], axis=0)
    turned = stack.astype(F32).T
    cols[...] = turned

    def column(m):
        return cols[:, m:m + 1]

    at_bound = 2 * per_slot + 2 * per_slot + 2 * per_node
    own_copy.wait()
    last = own_t[...].reshape(nodes, fw)
    share = sent.shape[1]
    for m in range(per_bound):
        spot = one_hot(column(at_bound + m).astype(jnp.int32), nodes)
        rows = jnp.dot(spot, last, preferred_element_type=F32)
        count = LANES // share
        sent[m * count:(m + 1) * count] = rows.reshape(count, share, fw).astype(BF16)
    lane = lax.broadcasted_iota(jnp.int32, (LANES, LANES), 1).astype(F32)
    table = cols[:, 2 * per_slot:4 * per_slot].astype(BF16)
    pair = lax.broadcasted_iota(jnp.int32, (LANES, 2 * per_slot), 1).astype(F32)
    for k in range(per_slot):
        low = (lane == column(k)).astype(F32).astype(BF16)
        found = jnp.dot(low, table, preferred_element_type=F32)
        high = column(per_slot + k)
        value = jnp.where(pair == high, found * LANES, jnp.where(pair == high + per_slot, found, 0.0))
        order[k * LANES:(k + 1) * LANES, 0:1] = jnp.sum(value, axis=1, keepdims=True)
    for k in range(per_node):
        marks = jnp.where(lane == 0, column(4 * per_slot + k),
                          jnp.where(lane == 1, column(4 * per_slot + per_node + k), 0.0))
        whole[k * LANES:(k + 1) * LANES, 3 * fw:4 * fw] = marks.astype(BF16)
    for k in range(3):
        feat_copy(k).wait()

    def batch_rows(i):
        rows_at = i * block + lax.broadcasted_iota(jnp.int32, (block, crow.shape[2]), 0)
        return rows_at // chunk == lax.broadcasted_iota(jnp.int32, (block, crow.shape[2]), 1)

    def gather_rows(i, own):
        at = rows_of(i)
        spot = one_hot(order[at, 0:1].astype(jnp.int32), nodes)
        pick[at, :] = spot
        rows = jnp.dot(pick[at, :], whole[...], preferred_element_type=F32)
        xs[at, 0:3 * fw] = rows[:, 0:3 * fw].astype(BF16)
        tags = rows[:, 3 * fw:4 * fw]
        tag[at, :] = tags
        return own + jnp.sum(jnp.where(batch_rows(i), tags[:, 1:2], 0.0), axis=0, keepdims=True)

    early = 2
    own_counts = lax.fori_loop(0, early, gather_rows, jnp.zeros((1, crow.shape[2]), F32))
    pl.semaphore_wait(barrier, n - 1)

    def send_halo(o):
        peer = lax.rem(me + o, n)
        return to(sent.at[peer], halo.at[me], p_s.at[0], p_r.at[0], peer // nrep, lax.rem(peer, nrep))

    def settle_all(src, dst, ssem, rsem):
        to(src.at[pl.ds(0, n - 1)], dst.at[pl.ds(0, n - 1)], ssem.at[0], rsem.at[0],
           chip * cores + other, rep).wait()

    def spread_weights(buf, sems):
        zsem, zrec, psem, prec, csem, crec = [sems.at[k] for k in range(6)]

        def along(o):
            return to(buf.at[rep, dom], buf.at[rep, dom], zsem, zrec, dom, lax.rem(rep + o, nrep))

        def across(p, o):
            at = lax.rem(rep + o, nrep)
            return to(buf.at[at, dom], buf.at[at, dom], psem, prec, plane(p) * cores + core, rep)

        def swap(p, o):
            at = lax.rem(rep + o, nrep)
            src = buf.at[at, lax.rem(chip - p + chips, chips) * cores + core]
            return to(src, src, csem, crec, chip * cores + other, rep)

        def each_pair(first, fn):
            each(chips, lambda p: each(nrep, lambda o: fn(p, o), 1), first)

        def settle(count, ssem, rsem):
            if count <= ndom:
                ref = buf.at[0, pl.ds(0, count)]
            else:
                ref = buf.at[pl.ds(0, nrep - 1), pl.ds(0, count // (nrep - 1))]
            to(ref, ref, ssem, rsem, chip * cores + other, rep).wait()

        def stage(s):
            if s == 0:
                each(nrep, lambda o: along(o).start(), 1)
            elif s == 1:
                settle(nrep - 1, zsem, zrec)
                each_pair(1, lambda p, o: across(p, o).start())
            elif s == 2:
                settle((nrep - 1) * (chips - 1), psem, prec)
                each_pair(0, lambda p, o: swap(p, o).start())
            else:
                settle((nrep - 1) * chips, csem, crec)
        return stage

    w1_stage = spread_weights(w1all, u_s)
    w2_stage = spread_weights(w2all, v_s)
    each(n, lambda o: send_halo(o).start(), 1)
    w1_stage(0)
    w2_stage(0)
    halo[me] = sent[me]

    own_counts = lax.fori_loop(early, steps, gather_rows, own_counts)
    w1_stage(1)
    w2_stage(1)
    crow[0] = own_counts
    cbuf[me] = own_counts

    def send_count(o):
        peer = lax.rem(me + o, n)
        return to(crow.at[0], cbuf.at[me], c_s.at[0], c_r.at[0], peer // nrep, lax.rem(peer, nrep))

    each(n, lambda o: send_count(o).start(), 1)

    def hop_near(i):
        left = jnp.concatenate([adjv[i, k] for k in range(kl)], axis=1)
        right = jnp.concatenate([own_t[lcols[i, k]] for k in range(kl)], axis=0)
        hacc[i] = jnp.dot(left, right, preferred_element_type=F32)

    def near_band(j):
        near_copy(j).wait()
        each((j + 1) * deep, hop_near, j * deep)

    each(bands, near_band)
    settle_all(sent, halo, p_s, p_r)
    halo_t[...] = halo[...].reshape(halo_t.shape)

    each(bands, lambda j: far_copy(j).wait())

    def hop_far(i):
        left = jnp.concatenate([adjv[i, kl + k] for k in range(kh)], axis=1)
        right = jnp.concatenate(
            [halo_t[hcols[k, i]] for k in range(kh)], axis=0)
        total = (hacc[i] + jnp.dot(left, right, preferred_element_type=F32)).astype(BF16)
        nh[pl.ds(pl.multiple_of(i * tile, tile), tile), :] = total
        next_out[pl.ds(pl.multiple_of(i * tile, tile), tile), :] = total

    each(row_tiles, hop_far)
    w1_stage(2)
    w2_stage(2)

    def gather_next(i):
        at = rows_of(i)
        xs[at, 3 * fw:4 * fw] = jnp.dot(pick[at, :], nh[...], preferred_element_type=F32).astype(BF16)

    each(steps, gather_next)
    w1_stage(3)

    def pre(i):
        at = rows_of(i)
        here = pl.ds(i * groups, groups)
        x = xs[at, :]
        for r in range(nrep):
            w1 = w1all[r].reshape(w1in.shape)
            z = jnp.dot(x, w1, preferred_element_type=F32)
            zs[at, r * width:(r + 1) * width] = z
            z3 = z.reshape(groups, chunk, width)
            mean = jnp.sum(z3, axis=1, keepdims=True) * (1.0 / chunk)
            off = z3 - mean
            spread2 = jnp.sum(off * off, axis=1, keepdims=True)
            for j in range(per):
                cut = slice(j * 128, (j + 1) * 128)
                fsrc[here, r * per + j:r * per + j + 1] = mean[:, :, cut]
                fsrc[here, half + r * per + j:half + r * per + j + 1] = spread2[:, :, cut]

    each(steps, pre)

    def chip_sum(src, got, part, xs_, xr, combine):
        def swap(a):
            return to(src.at[group_of(a, other)], got.at[a], xs_.at[0], xr.at[0], chip * cores + other, rep)

        def start():
            each(chips, lambda a: swap(a).start())

        def finish():
            to(part, got, xs_.at[0], xr.at[0], chip * cores + other, rep).wait()

            def one(a):
                part[a] = combine(src[group_of(a, core)], got[a])
            each(chips, one)
        return start, finish

    def walk(o):
        return lax.rem(chip + o // nrep, chips), lax.rem(rep + lax.rem(o, nrep), nrep)

    def scatter(part, arrived, as_, ar):
        def copy(o):
            a, r = walk(o)
            return to(part.at[a, r], arrived.at[o], as_.at[0], ar.at[0], a * cores + core, r)

        def start():
            each(peers, lambda o: copy(o).start(), 1)
            arrived[0] = part[chip, rep]

        def finish():
            span = arrived.at[pl.ds(0, peers - 1)]
            to(span, span, as_.at[0], ar.at[0], chip * cores + other, rep).wait()
        return start, finish

    def gather(gath, gs_, gr, ws, wr):
        def copy(o):
            a, r = walk(o)
            return to(gath.at[me], gath.at[me], gs_.at[0], gr.at[o // nrep], a * cores + core, r)

        def forward(da):
            at = group_of(lax.rem(chip + chips - da, chips), core)
            return to(gath.at[at], gath.at[at], ws.at[0], wr.at[0], chip * cores + other, rep)

        def settle(count, ssem, rsem):
            span = gath.at[pl.ds(0, count)]
            return to(span, span, ssem, rsem, chip * cores + other, rep)

        def start():
            each(peers, lambda o: copy(o).start(), 1)

        def finish():
            settle(nrep - 1, gs_.at[0], gr.at[0]).wait_recv()
            forward(0).start()

            def chip_in(da):
                settle(nrep, gs_.at[0], gr.at[da]).wait_recv()
                forward(da).start()
            each(chips, chip_in, 1)
            settle(peers, ws.at[0], wr.at[0]).wait()
            settle(peers - 1, gs_.at[0], gr.at[0]).wait_send()
        return start, finish

    def both_moments(a, b):
        ma, mb = a[:, :half], b[:, :half]
        gap = ma - mb
        spread2 = a[:, half:] + b[:, half:] + (0.5 * chunk) * gap * gap
        return jnp.concatenate([(ma + mb) * 0.5, spread2], axis=1)

    start, finish = chip_sum(fsrc, fin, fpart, fx_s, fx_r, both_moments)
    start()
    each(steps, lambda i: xt.__setitem__(
        (slice(None), pl.ds(pl.multiple_of(i * block, block), block)),
        xs[pl.ds(pl.multiple_of(i * block, block), block), :].T))
    finish()
    start, finish = scatter(fpart, fall, fa_s, fa_r)
    start()
    finish()
    got = fall[...]
    mu = jnp.sum(got[:, :half], axis=0) * (1.0 / peers)
    off = got[:, :half] - mu[None]
    m2 = jnp.sum(got[:, half:], axis=0) + (cores * chunk) * jnp.sum(off * off, axis=0)
    fgath[me] = jnp.concatenate([mu, lax.rsqrt(m2 * (1.0 / (n * chunk)) + 1e-05)], axis=0)
    start, finish = gather(fgath, fg_s, fg_r, fw_s, fw_r)
    start()
    loss_row = jnp.zeros((1, lrow.shape[2]), F32)
    w2_stage(3)
    settle_all(cbuf, cbuf, c_s, c_r)
    counts = jnp.maximum(jnp.sum(cbuf[...], axis=0), 1.0)
    finish()

    second = w2all[...].reshape(hidden_units, w2all.shape[3])

    def head(i, loss_row):
        at = pl.ds(pl.multiple_of(i * block, block), block)
        here = pl.ds(i * groups, groups)
        z3 = zs[at, :].reshape(groups, chunk, hidden_units)
        st = fgath[here]
        mean = jnp.concatenate([st[:, j:j + 1] for j in range(half)], axis=2)
        rstd = jnp.concatenate([st[:, half + j:half + j + 1] for j in range(half)], axis=2)
        normed = ((z3 - mean) * rstd).reshape(block, hidden_units)
        zs[at, :] = normed
        pick[at, 0:hidden_units] = jnp.maximum(normed, 0.0).astype(BF16)
        logits = jnp.dot(pick[at, 0:hidden_units], second, preferred_element_type=F32)
        lane = lax.broadcasted_iota(jnp.int32, logits.shape, 1)
        logits = jnp.where(lane < classes, logits, -1e30)
        row_max = jnp.max(logits, axis=1, keepdims=True)
        expos = jnp.exp(logits - row_max)
        totals = jnp.sum(expos, axis=1, keepdims=True)
        target = tag[at, 0:1].astype(jnp.int32)
        mark = tag[at, 1:2]
        onehot = (lane == target).astype(F32)
        cross = jnp.log(totals) + row_max - jnp.sum(onehot * logits, axis=1, keepdims=True)
        mine = batch_rows(i)
        count = jnp.sum(jnp.where(mine, counts, 0.0), axis=1, keepdims=True)
        dlogits = ((expos / totals - onehot) * (mark / count)).astype(BF16)
        pick[at, hidden_units:hidden_units + dlogits.shape[1]] = dlogits
        for r in range(nrep):
            span = slice(r * width, (r + 1) * width)
            seen = zs[at, span]
            back = by_lanes(dlogits, second[span])
            masked = jnp.where(seen > 0, back, 0.0)
            gs[at, span] = masked
            sums = jnp.sum(masked.reshape(groups, chunk, width), axis=1, keepdims=True)
            projs = jnp.sum((masked * seen).reshape(groups, chunk, width), axis=1, keepdims=True)
            for j in range(per):
                cut = slice(j * 128, (j + 1) * 128)
                bsrc[here, r * per + j:r * per + j + 1] = sums[:, :, cut]
                bsrc[here, half + r * per + j:half + r * per + j + 1] = projs[:, :, cut]
        return loss_row + jnp.sum(jnp.where(mine, mark * cross, 0.0), axis=0, keepdims=True)

    loss_row = lax.fori_loop(0, steps, head, loss_row)
    start, finish = chip_sum(bsrc, bin_, bpart, bx_s, bx_r, lambda a, b: a + b)
    start()
    loss_row = loss_row / jnp.maximum(own_counts, 1.0)
    lrow[0] = loss_row
    lbuf[me] = loss_row

    def send_loss(o):
        peer = lax.rem(me + o, n)
        return to(lrow.at[0], lbuf.at[me], l_s.at[0], l_r.at[0], peer // nrep, lax.rem(peer, nrep))

    part = hsrc.shape[3]
    for r in range(nrep):
        g2acc[r * width:(r + 1) * width, :] = lax.dot_general(
            pick[:, r * width:(r + 1) * width], pick[:, hidden_units:hidden_units + g2acc.shape[1]],
            (((0,), (0,)), ((), ())), preferred_element_type=F32)
        for d in range(ndom):
            first_row = (r * ndom + d) * part
            hsrc[d % cores, d // cores, r] = g2acc[first_row:first_row + part, :].astype(BF16)
    def h_near(o):
        return to(hsum.at[plane(o)], hnear.at[o - 1], hn_s.at[o], hn_r.at[o], plane(o) * cores + core, rep)

    def h_along(o):
        peer = lax.rem(rep + o, nrep)
        return to(hfar.at[peer], hfarin.at[o - 1], hf_s.at[o], hf_r.at[o], dom, peer)

    def h_round(o):
        return to(hgath.at[dom], hgath.at[dom], hg_s.at[o], hg_r.at[o], lax.rem(dom + o, ndom), rep)

    def h_stage(stage):
        if stage == 0:
            each(chips, lambda o: h_near(o).start(), 1)
        elif stage == 1:
            each(chips, lambda o: h_near(o).wait(), 1)
            total = hsrc[core, chip].astype(F32) + hin[chip].astype(F32)
            for o in range(1, chips):
                total = total + hnear[o - 1].astype(F32)
            hkeep[...] = total
            hfar[...] = total.astype(BF16)
            each(nrep, lambda o: h_along(o).start(), 1)
        elif stage == 2:
            each(nrep, lambda o: h_along(o).wait(), 1)
            total = hkeep[rep]
            for o in range(1, nrep):
                total = total + hfarin[o - 1].astype(F32)
            hgath[dom] = total
            each(ndom, lambda o: h_round(o).start(), 1)
        else:
            each(ndom, lambda o: h_round(o).wait(), 1)
            both = hgath[...].reshape(ndom * part, hgath.shape[2]).T
            second_out[...] = both[:classes]

    h_swap = to(hsrc.at[other], hin, hx_s.at[0], hx_r.at[0], chip * cores + other, rep)
    h_swap.start()
    finish()
    start, finish = scatter(bpart, ball, ba_s, ba_r)
    start()
    h_swap.wait()
    hsum[...] = (hsrc[core].astype(F32) + hin[...].astype(F32)).astype(BF16)
    h_stage(0)
    finish()
    bgath[me] = jnp.sum(ball[...], axis=0) * (1.0 / (n * chunk))
    start, finish = gather(bgath, bg_s, bg_r, bw_s, bw_r)
    start()
    each(n, lambda o: send_loss(o).start(), 1)
    h_stage(1)
    finish()

    high = acc.shape[0] // ndom

    def g_swap(r):
        return to(gsrc.at[r, other], gin.at[r], gx_s.at[r], gx_r.at[r], chip * cores + other, rep)

    def g_near(r, o):
        return to(gsum.at[r, plane(o)], gnear.at[r, o - 1], gn_s.at[r, o], gn_r.at[r, o],
                  plane(o) * cores + core, rep)

    def g_far(r):
        o = lax.rem(r - rep + nrep, nrep)
        return to(gfar.at[r], gfarin.at[o], gf_s.at[o], gf_r.at[o], dom, r)

    def g_stage(r, stage):
        if stage == 0:
            g_swap(r).start()
        elif stage == 1:
            g_swap(r).wait()
            gsum[r] = (gsrc[r, core].astype(F32) + gin[r].astype(F32)).astype(BF16)
            each(chips, lambda o: g_near(r, o).start(), 1)
        else:
            each(chips, lambda o: g_near(r, o).wait(), 1)
            total = gsrc[r, core, chip].astype(F32) + gin[r, chip].astype(F32)
            for o in range(1, chips):
                total = total + gnear[r, o - 1].astype(F32)
            gkeep[r] = total
            gfar[r] = total.astype(BF16)

            @pl.when(rep != r)
            def _():
                g_far(r).start()

    def tail(r):
        cols = slice(r * width, (r + 1) * width)

        def block_dz(i):
            at = pl.ds(pl.multiple_of(i * block, block), block)
            here = pl.ds(i * groups, groups)
            low = r * per

            def lines(ref, first):
                return jnp.concatenate(
                    [ref[here, first + j:first + j + 1] for j in range(per)], axis=2)

            masked = gs[at, cols].reshape(groups, chunk, width)
            normed = zs[at, cols].reshape(groups, chunk, width)
            dz = (masked - lines(bgath, low) - normed * lines(bgath, half + low)) * lines(fgath, half + low)
            dzs[at, :] = dz.reshape(block, width).astype(BF16)

        each(steps, block_dz)
        acc[...] = jnp.dot(xt[...], dzs[...], preferred_element_type=F32)
        for d in range(ndom):
            gsrc[r, d % cores, d // cores] = acc[d * high:(d + 1) * high, :].astype(BF16)

    for r in range(nrep):
        tail(r)
        if r == 1:
            h_stage(2)
        g_stage(r, 0)
        if r >= 1:
            g_stage(r - 1, 1)
        if r >= 2:
            g_stage(r - 2, 2)
    if nrep < 2:
        h_stage(2)
    g_stage(nrep - 1, 1)
    if nrep >= 2:
        g_stage(nrep - 2, 2)
    h_stage(3)
    settle_all(lbuf, lbuf, l_s, l_r)
    losses = lbuf[...]
    source = lax.broadcasted_iota(jnp.int32, losses.shape, 0)
    lane = lax.broadcasted_iota(jnp.int32, losses.shape, 2)
    mine = jnp.sum(jnp.where(lane == me, losses, 0.0), axis=2, keepdims=True)
    loss_out[...] = jnp.sum(jnp.where(lane == source, mine, 0.0), axis=0)[:, :n]
    g_stage(nrep - 1, 2)

    def g_own(o):
        return to(gfar.at[rep], gfarin.at[o], gf_s.at[o], gf_r.at[o], dom, lax.rem(rep + o, nrep))

    each(nrep, lambda o: g_own(o).wait_recv(), 1)
    total = gkeep[rep]
    for o in range(1, nrep):
        total = total + gfarin[o].astype(F32)
    first_out[...] = total
    each(nrep, lambda o: g_own(o).wait_send(), 1)


def hop_kernel(kl, kh, lcols, hcols, adj_l, adj_h, own, halo, out):
    i = pl.program_id(0)
    left = jnp.concatenate([adj_l[0, k] for k in range(kl)] + [adj_h[0, k] for k in range(kh)], axis=1)
    right = jnp.concatenate(
        [own[0, lcols[i, k]] for k in range(kl)] + [halo[hcols[i, k]] for k in range(kh)], axis=0)
    out[0] = jnp.dot(left, right, preferred_element_type=F32).astype(BF16)


def batch_lanes(rows, wide, chunk):
    at = pl.program_id(0) * rows + lax.broadcasted_iota(jnp.int32, (rows, wide), 0)
    return at // chunk == lax.broadcasted_iota(jnp.int32, (rows, wide), 1)


def one_hot(column, count):
    lanes = lax.broadcasted_iota(jnp.int32, (column.shape[0], count), 1)
    return (lanes == column).astype(F32).astype(BF16)


def by_lanes(left, right):
    return lax.dot_general(left, right, (((1,), (1,)), ((), ())), preferred_element_type=F32)


def pick_kernel(chunk, shuf, bound, ids, labels, labelled, feats, x_out, tag_out, sent_out, cnt_out):
    rows = shuf.shape[0]
    nodes = feats.shape[1]
    sent_out[...] = jnp.dot(one_hot(bound[...], nodes), feats[2], preferred_element_type=F32).astype(BF16)
    numbers = ids[...]
    blank = jnp.zeros((6, nodes), F32)
    table = jnp.concatenate(
        [(numbers // 256).astype(F32), (numbers % 256).astype(F32), jnp.zeros((6, ids.shape[1]), F32)], axis=0)
    two = by_lanes(one_hot(shuf[...], ids.shape[1]), table.astype(BF16))
    order = two[:, 0:1] * 256.0 + two[:, 1:2]
    pick = one_hot(order.astype(jnp.int32), nodes)
    whole = jnp.concatenate([feats[0], feats[1], feats[2]], axis=1)
    x_out[...] = jnp.dot(pick, whole, preferred_element_type=F32).astype(BF16)
    marks = jnp.concatenate([labels[...].astype(F32), labelled[...].astype(F32), blank], axis=0)
    tags = by_lanes(pick, marks.astype(BF16))
    tag_out[:, 0:8] = tags
    tag_out[:, 8:9] = order

    @pl.when(pl.program_id(0) == 0)
    def _():
        cnt_out[...] = jnp.zeros_like(cnt_out)

    here = batch_lanes(rows, cnt_out.shape[1], chunk)
    cnt_out[...] += jnp.sum(jnp.where(here, tags[:, 1:2], 0.0), axis=0, keepdims=True)


def emit_kernel(*refs):
    count = len(refs) // 2
    for source, target in zip(refs[:count], refs[count:]):
        target[...] = source[...]


def dma_sems(n, count):
    return [pltpu.SemaphoreType.DMA((n,))] * count


def shards(hop_feats, adj_local, local_cols, adj_halo, halo_cols, boundary_rows, train_ids,
           shuffle, labels, labelled, w_first, w_second):
    ndom, nrep = lax.axis_size("dom"), lax.axis_size("rep")
    n = ndom * nrep
    cores = 2
    row_tiles, kl, tile, _ = adj_local.shape
    kh = adj_halo.shape[1]
    nodes, width = hop_feats.shape[1:]
    slots = train_ids.shape[1]
    hidden_units, classes = w_second.shape[0] * nrep, w_second.shape[1]
    chunk = slots // n
    wide = -(-n // LANES) * LANES
    sds = jax.ShapeDtypeStruct
    own_cols = hidden_units // nrep
    span = -(-classes // LANES) * LANES
    lines = 2 * hidden_units // LANES
    chips = ndom // cores
    peers = chips * nrep
    own_rows, part = 4 * width // ndom, hidden_units // n
    share = boundary_rows.shape[1] // n
    vm = pltpu.VMEM

    def moment_scratch():
        return [vm((n, lines, LANES), F32), vm((chips, nrep, lines, LANES), F32),
                vm((chips, nrep, lines, LANES), F32), vm((peers, lines, LANES), F32), vm((n, lines, LANES), F32)]

    def pairs(a, b, count):
        return [pltpu.SemaphoreType.DMA((a, b))] * count

    grad_block = (own_rows, own_cols)
    half_block = (part, span)
    scratch = [
        vm((8, max(slots, nodes)), jnp.int32), vm((LANES, LANES), F32), vm((slots, LANES), F32),
        vm((nodes, 4 * width), BF16), vm((row_tiles, kl + kh, tile, tile), BF16),
        vm((row_tiles, tile, width), F32), vm((nodes, width), BF16), vm((slots, nodes), BF16),
        vm((n, share, width), BF16), vm((n, share, width), BF16), vm((row_tiles, tile, width), BF16),
        vm((n * share // tile, tile, width), BF16), vm((slots, width), F32),
        vm((nrep, ndom, 4 * width // ndom, own_cols), BF16),
        vm((nrep, ndom, own_cols // ndom, span), BF16),
        vm((span, own_cols), F32), vm((1, 1, wide), F32), vm((n, 1, wide), F32),
    ]
    bands = 4 if row_tiles % 4 == 0 else row_tiles
    scratch += dma_sems(3, 1) + dma_sems(1, 1) + dma_sems(bands, 2) + dma_sems(5, 1) + dma_sems(1, 4)
    scratch += dma_sems(6, 2)
    scratch += [
        vm((slots, 4 * width), BF16), vm((4 * width, slots), BF16), vm((slots, hidden_units), F32),
        vm((slots, hidden_units), F32), vm((slots, own_cols), BF16), vm((hidden_units, span), F32),
        vm((4 * width, own_cols), F32), vm((1, 1, wide), F32), vm((n, 1, wide), F32),
        *moment_scratch(), *moment_scratch(),
        vm((nrep, cores, chips) + grad_block, BF16), vm((nrep, chips) + grad_block, BF16),
        vm((nrep, chips) + grad_block, BF16), vm((nrep, chips - 1) + grad_block, BF16),
        vm((nrep,) + grad_block, BF16), vm((nrep,) + grad_block, F32), vm((nrep,) + grad_block, BF16),
        vm((cores, chips, nrep) + half_block, BF16), vm((chips, nrep) + half_block, BF16),
        vm((chips, nrep) + half_block, BF16), vm((chips - 1, nrep) + half_block, BF16),
        vm((nrep,) + half_block, F32), vm((nrep,) + half_block, BF16), vm((nrep - 1,) + half_block, BF16),
        vm((ndom,) + half_block, F32),
    ]
    moment_sems = dma_sems(1, 5) + dma_sems(chips, 1) + dma_sems(1, 2)
    scratch += moment_sems + moment_sems + dma_sems(1, 2) + dma_sems(nrep, 2)
    scratch += pairs(nrep, chips, 2) + dma_sems(nrep, 2)
    scratch += dma_sems(1, 2) + dma_sems(chips, 2) + dma_sems(nrep, 2) + dma_sems(ndom, 2)
    vmem = pl.BlockSpec(memory_space=pltpu.VMEM)
    smem = pl.BlockSpec(memory_space=pltpu.SMEM)
    where = pl.BlockSpec(memory_space=pl.ANY)
    next_hop, first, second, loss = pl.pallas_call(
        functools.partial(step_kernel, chunk, ndom, nrep, cores, classes, kl, kh),
        out_shape=(sds((nodes, width), BF16), sds((own_rows, own_cols), F32),
                   sds((classes, own_cols), F32), sds((1, n), F32)),
        in_specs=[smem, smem, vmem, vmem] + [where] * 9,
        out_specs=(vmem, vmem, vmem, vmem),
        scratch_shapes=scratch,
        compiler_params=pltpu.CompilerParams(collective_id=2, has_side_effects=True, vmem_limit_bytes=BIG),
        name="step",
    )(local_cols, halo_cols.T, w_first, w_second.T, hop_feats, adj_local, adj_halo,
      hop_feats.reshape(3, row_tiles, tile, width), boundary_rows,
      train_ids, shuffle, labels[None], labelled[None])
    done = (next_hop, loss, first, second)
    specs = [pl.BlockSpec(v.shape, lambda i: (0, 0)) for v in done]
    next_hop, loss, first, second = pl.pallas_call(
        emit_kernel,
        out_shape=tuple(sds(v.shape, v.dtype) for v in done),
        grid=(1,),
        in_specs=specs,
        out_specs=tuple(specs),
        name="emit",
    )(*done)
    return (next_hop, loss, first, second.T)


def solution(mesh):
    both = ("dom", "rep")
    placed = (
        P(None, both, None), P(both, None, None, None), P(both, None), P(both, None, None, None),
        P(both, None), P(both, None), P(both, None), P(both, None), P(both), P(both),
        P(None, "rep"), P("rep", None),
    )
    return jax.shard_map(
        shards, mesh=mesh, in_specs=placed,
        out_specs=(P(both, None), P(both, None), P("dom", "rep"), P("rep", None)),
        check_vma=False,
    )
```

```python
import functools

import jax
import jax.numpy as jnp
from jax import lax
from jax.experimental import pallas as pl
from jax.experimental.pallas import tpu as pltpu
from jax.sharding import PartitionSpec as P

F32 = jnp.float32
BF16 = jnp.bfloat16
BIG = 63 * 1024 * 1024
LANES = 128


def one_hot(column, count):
    lanes = lax.broadcasted_iota(jnp.int32, (column.shape[0], count), 1)
    return (lanes == column).astype(F32).astype(BF16)


def by_lanes(left, right):
    return lax.dot_general(left, right, (((1,), (1,)), ((), ())), preferred_element_type=F32)


def step_kernel(chunk, ndom, nrep, cores, classes, kl, kh,
               lcols, hcols, w1in, w2in, feats, adj_l, adj_h, tiles, bound, ids, shuf, labels, labelled,
               next_out, first_out, second_out, loss_out,
               ints, cols, order, whole, adjv, hacc, nh, pick, sent, halo, own_t, halo_t, tag, w1all, w2all, w2t, crow, cbuf,
               f_s, t_s, a_s, b_s, i_s, c_s, c_r, p_s, p_r, u_s, v_s,
               xs, xt, zs, gs, dzs, g2acc, acc, lrow, lbuf,
               fsrc, fin, fpart, fall, fgath, bsrc, bin_, bpart, ball, bgath,
               gsrc, gin, gsum, gnear, gfar, gkeep, gfarin,
               hsrc, hin, hsum, hnear, hkeep, hfar, hfarin, hgath,
               fx_s, fx_r, fa_s, fa_r, fg_s, fg_r, fw_s, fw_r,
               bx_s, bx_r, ba_s, ba_r, bg_s, bg_r, bw_s, bw_r,
               l_s, l_r, gx_s, gx_r, gn_s, gn_r, gf_s, gf_r,
               hx_s, hx_r, hn_s, hn_r, hf_s, hf_r, hg_s, hg_r):
    n = ndom * nrep
    chips = ndom // cores
    peers = chips * nrep
    dom, rep = lax.axis_index("dom"), lax.axis_index("rep")
    me = dom * nrep + rep
    chip, core = dom // cores, lax.rem(dom, cores)
    other = cores - 1 - core
    block = 256
    slots, hidden_units = zs.shape
    steps = slots // block
    groups = block // chunk
    half = fsrc.shape[1] // 2
    width = hidden_units // nrep
    per = half // nrep

    barrier = pltpu.get_barrier_semaphore()

    def greet(o, carry):
        peer = lax.rem(me + o, n)
        pl.semaphore_signal(barrier, inc=1, device_id=(peer // nrep, lax.rem(peer, nrep)),
                            device_id_type=pl.DeviceIdType.MESH)
        return carry

    lax.fori_loop(1, n, greet, 0)

    def to(src, dst, ssem, rsem, peer_dom, peer_rep):
        return pltpu.make_async_remote_copy(
            src_ref=src, dst_ref=dst, send_sem=ssem, recv_sem=rsem,
            device_id=(peer_dom, peer_rep), device_id_type=pl.DeviceIdType.MESH)

    def each(count, fn, first=0):
        lax.fori_loop(first, count, lambda i, carry: (fn(i), carry)[1], 0)

    def group_of(a, c):
        return pl.ds((a * cores + c) * nrep, nrep)

    def plane(o):
        return lax.rem(chip + o, chips)

    def rows_of(i):
        return pl.ds(pl.multiple_of(i * block, block), block)

    row_tiles, tile, fw = hacc.shape
    nodes = whole.shape[0]

    def feat_copy(k):
        return pltpu.make_async_copy(feats.at[k], whole.at[:, k * fw:(k + 1) * fw], f_s.at[k])

    bands = a_s.shape[0]
    deep = row_tiles // bands

    def near_copy(j):
        at = pl.ds(j * deep, deep)
        return pltpu.make_async_copy(adj_l.at[at], adjv.at[at, 0:kl], a_s.at[j])

    def far_copy(j):
        at = pl.ds(j * deep, deep)
        return pltpu.make_async_copy(adj_h.at[at], adjv.at[at, kl:kl + kh], b_s.at[j])

    given = (shuf, ids, labels, labelled, bound)
    int_copies = [pltpu.make_async_copy(ref, ints.at[m:m + 1, 0:ref.shape[1]], i_s.at[m])
                  for m, ref in enumerate(given)]
    for copy in int_copies:
        copy.start()
    own_copy = pltpu.make_async_copy(tiles.at[2], own_t, t_s.at[0])
    own_copy.start()
    feat_copy(2).start()
    feat_copy(0).start()
    feat_copy(1).start()
    each(bands, lambda j: near_copy(j).start())
    each(bands, lambda j: far_copy(j).start())

    w1all[rep] = w1in[...].reshape(w1all.shape[1:])
    w2t[...] = jnp.zeros_like(w2t)
    w2t[0:classes, :] = w2in[...].astype(F32)
    w2all[rep] = w2t[...].T.astype(BF16).reshape(w2all.shape[1:])
    for copy in int_copies:
        copy.wait()

    def lines_of(m, count):
        return jnp.concatenate([ints[m:m + 1, j * LANES:(j + 1) * LANES] for j in range(count)], axis=0)

    per_slot, per_node, per_bound = slots // LANES, nodes // LANES, bound.shape[1] // LANES
    shuf_lines, id_lines = lines_of(0, per_slot), lines_of(1, per_slot)
    stack = [shuf_lines % LANES, shuf_lines // LANES, id_lines // LANES, id_lines % LANES,
             lines_of(2, per_node), lines_of(3, per_node), lines_of(4, per_bound)]
    used = sum(s.shape[0] for s in stack)
    stack = jnp.concatenate(stack + [jnp.zeros((LANES - used, LANES), jnp.int32)], axis=0)
    turned = stack.astype(F32).T
    cols[...] = turned

    def column(m):
        return cols[:, m:m + 1]

    at_bound = 2 * per_slot + 2 * per_slot + 2 * per_node
    own_copy.wait()
    last = own_t[...].reshape(nodes, fw)
    share = sent.shape[1]
    for m in range(per_bound):
        spot = one_hot(column(at_bound + m).astype(jnp.int32), nodes)
        rows = jnp.dot(spot, last, preferred_element_type=F32)
        count = LANES // share
        sent[m * count:(m + 1) * count] = rows.reshape(count, share, fw).astype(BF16)
    lane = lax.broadcasted_iota(jnp.int32, (LANES, LANES), 1).astype(F32)
    table = cols[:, 2 * per_slot:4 * per_slot].astype(BF16)
    pair = lax.broadcasted_iota(jnp.int32, (LANES, 2 * per_slot), 1).astype(F32)
    for k in range(per_slot):
        low = (lane == column(k)).astype(F32).astype(BF16)
        found = jnp.dot(low, table, preferred_element_type=F32)
        high = column(per_slot + k)
        value = jnp.where(pair == high, found * LANES, jnp.where(pair == high + per_slot, found, 0.0))
        order[k * LANES:(k + 1) * LANES, 0:1] = jnp.sum(value, axis=1, keepdims=True)
    for k in range(per_node):
        marks = jnp.where(lane == 0, column(4 * per_slot + k),
                          jnp.where(lane == 1, column(4 * per_slot + per_node + k), 0.0))
        whole[k * LANES:(k + 1) * LANES, 3 * fw:4 * fw] = marks.astype(BF16)
    for k in range(3):
        feat_copy(k).wait()

    def batch_rows(i, count):
        rows_at = i * count + lax.broadcasted_iota(jnp.int32, (count, crow.shape[2]), 0)
        return rows_at // chunk == lax.broadcasted_iota(jnp.int32, (count, crow.shape[2]), 1)

    def gather_rows(i, own):
        at = rows_of(i)
        spot = order[at, 0:1].astype(jnp.int32)
        strip = 2 * LANES
        for j in range(nodes // strip):
            pick[at, j * strip:(j + 1) * strip] = one_hot(spot - j * strip, strip)
        rows = jnp.dot(pick[at, :], whole[...], preferred_element_type=F32)
        xs[at, 0:3 * fw] = rows[:, 0:3 * fw].astype(BF16)
        tags = rows[:, 3 * fw:4 * fw]
        tag[at, :] = tags
        return own + jnp.sum(jnp.where(batch_rows(i, block), tags[:, 1:2], 0.0), axis=0, keepdims=True)

    early = 2
    own_counts = lax.fori_loop(0, early, gather_rows, jnp.zeros((1, crow.shape[2]), F32))
    pl.semaphore_wait(barrier, n - 1)

    def send_halo(o):
        peer = lax.rem(me + o, n)
        return to(sent.at[peer], halo.at[me], p_s.at[0], p_r.at[0], peer // nrep, lax.rem(peer, nrep))

    def settle_all(src, dst, ssem, rsem):
        to(src.at[pl.ds(0, n - 1)], dst.at[pl.ds(0, n - 1)], ssem.at[0], rsem.at[0],
           chip * cores + other, rep).wait()

    def spread_weights(buf, sems):
        zsem, zrec, psem, prec, csem, crec = [sems.at[k] for k in range(6)]

        def along(o):
            return to(buf.at[rep, dom], buf.at[rep, dom], zsem, zrec, dom, lax.rem(rep + o, nrep))

        def across(p, o):
            at = lax.rem(rep + o, nrep)
            return to(buf.at[at, dom], buf.at[at, dom], psem, prec, plane(p) * cores + core, rep)

        def swap(p, o):
            at = lax.rem(rep + o, nrep)
            src = buf.at[at, lax.rem(chip - p + chips, chips) * cores + core]
            return to(src, src, csem, crec, chip * cores + other, rep)

        def each_pair(first, fn):
            each(chips, lambda p: each(nrep, lambda o: fn(p, o), 1), first)

        def settle(count, ssem, rsem):
            if count <= ndom:
                ref = buf.at[0, pl.ds(0, count)]
            else:
                ref = buf.at[pl.ds(0, nrep - 1), pl.ds(0, count // (nrep - 1))]
            to(ref, ref, ssem, rsem, chip * cores + other, rep).wait()

        def stage(s):
            if s == 0:
                each(nrep, lambda o: along(o).start(), 1)
            elif s == 1:
                settle(nrep - 1, zsem, zrec)
                each_pair(1, lambda p, o: across(p, o).start())
            elif s == 2:
                settle((nrep - 1) * (chips - 1), psem, prec)
                each_pair(0, lambda p, o: swap(p, o).start())
            else:
                settle((nrep - 1) * chips, csem, crec)
        return stage

    w1_stage = spread_weights(w1all, u_s)
    w2_stage = spread_weights(w2all, v_s)
    each(n, lambda o: send_halo(o).start(), 1)
    w1_stage(0)
    w2_stage(0)
    halo[me] = sent[me]

    own_counts = lax.fori_loop(early, steps, gather_rows, own_counts)
    w1_stage(1)
    crow[0] = own_counts
    cbuf[me] = own_counts

    def send_count(o):
        peer = lax.rem(me + o, n)
        return to(crow.at[0], cbuf.at[me], c_s.at[0], c_r.at[0], peer // nrep, lax.rem(peer, nrep))

    each(n, lambda o: send_count(o).start(), 1)

    def hop_near(i):
        left = jnp.concatenate([adjv[i, k] for k in range(kl)], axis=1)
        right = jnp.concatenate([own_t[lcols[i, k]] for k in range(kl)], axis=0)
        hacc[i] = jnp.dot(left, right, preferred_element_type=F32)

    def near_band(j):
        near_copy(j).wait()
        each((j + 1) * deep, hop_near, j * deep)

    each(bands, near_band)
    settle_all(sent, halo, p_s, p_r)
    halo_t[...] = halo[...].reshape(halo_t.shape)

    each(bands, lambda j: far_copy(j).wait())

    def hop_far(i):
        left = jnp.concatenate([adjv[i, kl + k] for k in range(kh)], axis=1)
        right = jnp.concatenate(
            [halo_t[hcols[k, i]] for k in range(kh)], axis=0)
        total = (hacc[i] + jnp.dot(left, right, preferred_element_type=F32)).astype(BF16)
        nh[pl.ds(pl.multiple_of(i * tile, tile), tile), :] = total
        next_out[pl.ds(pl.multiple_of(i * tile, tile), tile), :] = total

    each(row_tiles, hop_far)
    w1_stage(2)
    w2_stage(1)

    def gather_next(i):
        at = rows_of(i)
        xs[at, 3 * fw:4 * fw] = jnp.dot(pick[at, :], nh[...], preferred_element_type=F32).astype(BF16)

    each(steps, gather_next)
    w1_stage(3)

    def pre(i):
        at = rows_of(i)
        here = pl.ds(i * groups, groups)
        x = xs[at, :]
        for r in range(nrep):
            w1 = w1all[r].reshape(w1in.shape)
            z = jnp.dot(x, w1, preferred_element_type=F32)
            zs[at, r * width:(r + 1) * width] = z
            z3 = z.reshape(groups, chunk, width)
            mean = jnp.sum(z3, axis=1, keepdims=True) * (1.0 / chunk)
            off = z3 - mean
            spread2 = jnp.sum(off * off, axis=1, keepdims=True)
            for j in range(per):
                cut = slice(j * 128, (j + 1) * 128)
                fsrc[here, r * per + j:r * per + j + 1] = mean[:, :, cut]
                fsrc[here, half + r * per + j:half + r * per + j + 1] = spread2[:, :, cut]

    each(steps, pre)
    w2_stage(2)

    def chip_sum(src, got, part, xs_, xr, combine):
        def swap(a):
            return to(src.at[group_of(a, other)], got.at[a], xs_.at[0], xr.at[0], chip * cores + other, rep)

        def start():
            each(chips, lambda a: swap(a).start())

        def finish():
            to(part, got, xs_.at[0], xr.at[0], chip * cores + other, rep).wait()

            def one(a):
                part[a] = combine(src[group_of(a, core)], got[a])
            each(chips, one)
        return start, finish

    def walk(o):
        return lax.rem(chip + o // nrep, chips), lax.rem(rep + lax.rem(o, nrep), nrep)

    def scatter(part, arrived, as_, ar):
        def copy(o):
            a, r = walk(o)
            return to(part.at[a, r], arrived.at[o], as_.at[0], ar.at[0], a * cores + core, r)

        def start():
            each(peers, lambda o: copy(o).start(), 1)
            arrived[0] = part[chip, rep]

        def finish():
            span = arrived.at[pl.ds(0, peers - 1)]
            to(span, span, as_.at[0], ar.at[0], chip * cores + other, rep).wait()
        return start, finish

    def gather(gath, gs_, gr, ws, wr):
        def copy(o):
            a, r = walk(o)
            return to(gath.at[me], gath.at[me], gs_.at[0], gr.at[o // nrep], a * cores + core, r)

        def forward(da):
            at = group_of(lax.rem(chip + chips - da, chips), core)
            return to(gath.at[at], gath.at[at], ws.at[0], wr.at[0], chip * cores + other, rep)

        def settle(count, ssem, rsem):
            span = gath.at[pl.ds(0, count)]
            return to(span, span, ssem, rsem, chip * cores + other, rep)

        def start():
            each(peers, lambda o: copy(o).start(), 1)

        def finish():
            settle(nrep - 1, gs_.at[0], gr.at[0]).wait_recv()
            forward(0).start()

            def chip_in(da):
                settle(nrep, gs_.at[0], gr.at[da]).wait_recv()
                forward(da).start()
            each(chips, chip_in, 1)
            settle(peers, ws.at[0], wr.at[0]).wait()
            settle(peers - 1, gs_.at[0], gr.at[0]).wait_send()
        return start, finish

    def both_moments(a, b):
        ma, mb = a[:, :half], b[:, :half]
        gap = ma - mb
        spread2 = a[:, half:] + b[:, half:] + (0.5 * chunk) * gap * gap
        return jnp.concatenate([(ma + mb) * 0.5, spread2], axis=1)

    start, finish = chip_sum(fsrc, fin, fpart, fx_s, fx_r, both_moments)
    start()
    each(steps, lambda i: xt.__setitem__(
        (slice(None), pl.ds(pl.multiple_of(i * block, block), block)),
        xs[pl.ds(pl.multiple_of(i * block, block), block), :].T))
    finish()
    start, finish = scatter(fpart, fall, fa_s, fa_r)
    start()
    finish()
    got = fall[...]
    mu = jnp.sum(got[:, :half], axis=0) * (1.0 / peers)
    off = got[:, :half] - mu[None]
    m2 = jnp.sum(got[:, half:], axis=0) + (cores * chunk) * jnp.sum(off * off, axis=0)
    fgath[me] = jnp.concatenate([mu, lax.rsqrt(m2 * (1.0 / (n * chunk)) + 1e-05)], axis=0)
    start, finish = gather(fgath, fg_s, fg_r, fw_s, fw_r)
    start()
    loss_row = jnp.zeros((1, lrow.shape[2]), F32)
    w2_stage(3)
    settle_all(cbuf, cbuf, c_s, c_r)
    counts = jnp.maximum(jnp.sum(cbuf[...], axis=0), 1.0)
    finish()


    few = block
    some = few // chunk

    def head_rows(i):
        at = pl.ds(pl.multiple_of(i * few, few), few)
        here = pl.ds(i * some, some)
        st = fgath[here]
        for r in range(nrep):
            span = slice(r * width, (r + 1) * width)
            z3 = zs[at, span].reshape(some, chunk, width)
            mean = jnp.concatenate([st[:, r * per + j:r * per + j + 1] for j in range(per)], axis=2)
            rstd = jnp.concatenate(
                [st[:, half + r * per + j:half + r * per + j + 1] for j in range(per)], axis=2)
            normed = ((z3 - mean) * rstd).reshape(few, width)
            zs[at, span] = normed
            pick[at, span] = jnp.maximum(normed, 0.0).astype(BF16)
        second = w2all[...].reshape(hidden_units, w2all.shape[3])
        logits = jnp.dot(pick[at, 0:hidden_units], second, preferred_element_type=F32)
        lane = lax.broadcasted_iota(jnp.int32, logits.shape, 1)
        logits = jnp.where(lane < classes, logits, -1e30)
        row_max = jnp.max(logits, axis=1, keepdims=True)
        expos = jnp.exp(logits - row_max)
        totals = jnp.sum(expos, axis=1, keepdims=True)
        target = tag[at, 0:1].astype(jnp.int32)
        mark = tag[at, 1:2]
        onehot = (lane == target).astype(F32)
        cross = jnp.log(totals) + row_max - jnp.sum(onehot * logits, axis=1, keepdims=True)
        mine = batch_rows(i, few)
        count = jnp.sum(jnp.where(mine, counts, 0.0), axis=1, keepdims=True)
        dlogits = ((expos / totals - onehot) * (mark / count)).astype(BF16)
        pick[at, hidden_units:hidden_units + dlogits.shape[1]] = dlogits
        for r in range(nrep):
            span = slice(r * width, (r + 1) * width)
            seen = zs[at, span]
            back = by_lanes(dlogits, w2all[r].reshape(width, w2all.shape[3]))
            masked = jnp.where(seen > 0, back, 0.0)
            gs[at, span] = masked
            sums = jnp.sum(masked.reshape(some, chunk, width), axis=1, keepdims=True)
            projs = jnp.sum((masked * seen).reshape(some, chunk, width), axis=1, keepdims=True)
            for j in range(per):
                cut = slice(j * 128, (j + 1) * 128)
                bsrc[here, r * per + j:r * per + j + 1] = sums[:, :, cut]
                bsrc[here, half + r * per + j:half + r * per + j + 1] = projs[:, :, cut]
        return jnp.sum(jnp.where(mine, mark * cross, 0.0), axis=0, keepdims=True)

    def head(i, loss_row):
        for k in range(block // few):
            loss_row = loss_row + head_rows(i * (block // few) + k)
        return loss_row

    loss_row = lax.fori_loop(0, steps, head, loss_row)
    start, finish = chip_sum(bsrc, bin_, bpart, bx_s, bx_r, lambda a, b: a + b)
    start()
    loss_row = loss_row / jnp.maximum(own_counts, 1.0)
    lrow[0] = loss_row
    lbuf[me] = loss_row

    def send_loss(o):
        peer = lax.rem(me + o, n)
        return to(lrow.at[0], lbuf.at[me], l_s.at[0], l_r.at[0], peer // nrep, lax.rem(peer, nrep))

    part = hsrc.shape[3]
    for r in range(nrep):
        g2acc[r * width:(r + 1) * width, :] = lax.dot_general(
            pick[:, r * width:(r + 1) * width], pick[:, hidden_units:hidden_units + g2acc.shape[1]],
            (((0,), (0,)), ((), ())), preferred_element_type=F32)
        for d in range(ndom):
            first_row = (r * ndom + d) * part
            hsrc[d % cores, d // cores, r] = g2acc[first_row:first_row + part, :].astype(BF16)
    def h_near(o):
        return to(hsum.at[plane(o)], hnear.at[o - 1], hn_s.at[o], hn_r.at[o], plane(o) * cores + core, rep)

    def h_along(o):
        peer = lax.rem(rep + o, nrep)
        return to(hfar.at[peer], hfarin.at[o - 1], hf_s.at[o], hf_r.at[o], dom, peer)

    def h_round(o):
        return to(hgath.at[dom], hgath.at[dom], hg_s.at[o], hg_r.at[o], lax.rem(dom + o, ndom), rep)

    def h_stage(stage):
        if stage == 0:
            each(chips, lambda o: h_near(o).start(), 1)
        elif stage == 1:
            each(chips, lambda o: h_near(o).wait(), 1)
            total = hsrc[core, chip].astype(F32) + hin[chip].astype(F32)
            for o in range(1, chips):
                total = total + hnear[o - 1].astype(F32)
            hkeep[...] = total
            hfar[...] = total.astype(BF16)
            each(nrep, lambda o: h_along(o).start(), 1)
        elif stage == 2:
            each(nrep, lambda o: h_along(o).wait(), 1)
            total = hkeep[rep]
            for o in range(1, nrep):
                total = total + hfarin[o - 1].astype(F32)
            hgath[dom] = total
            each(ndom, lambda o: h_round(o).start(), 1)
        else:
            each(ndom, lambda o: h_round(o).wait(), 1)
            both = hgath[...].reshape(ndom * part, hgath.shape[2]).T
            second_out[...] = both[:classes]

    h_swap = to(hsrc.at[other], hin, hx_s.at[0], hx_r.at[0], chip * cores + other, rep)
    h_swap.start()
    finish()
    start, finish = scatter(bpart, ball, ba_s, ba_r)
    start()
    h_swap.wait()
    hsum[...] = (hsrc[core].astype(F32) + hin[...].astype(F32)).astype(BF16)
    h_stage(0)
    finish()
    bgath[me] = jnp.sum(ball[...], axis=0) * (1.0 / (n * chunk))
    start, finish = gather(bgath, bg_s, bg_r, bw_s, bw_r)
    start()
    each(n, lambda o: send_loss(o).start(), 1)
    h_stage(1)
    finish()

    high = acc.shape[0] // ndom

    def g_swap(r):
        return to(gsrc.at[r, other], gin.at[r], gx_s.at[r], gx_r.at[r], chip * cores + other, rep)

    def g_near(r, o):
        return to(gsum.at[r, plane(o)], gnear.at[r, o - 1], gn_s.at[r, o], gn_r.at[r, o],
                  plane(o) * cores + core, rep)

    def g_far(r):
        o = lax.rem(r - rep + nrep, nrep)
        return to(gfar.at[r], gfarin.at[o], gf_s.at[o], gf_r.at[o], dom, r)

    def g_stage(r, stage):
        if stage == 0:
            g_swap(r).start()
        elif stage == 1:
            g_swap(r).wait()
            gsum[r] = (gsrc[r, core].astype(F32) + gin[r].astype(F32)).astype(BF16)
            each(chips, lambda o: g_near(r, o).start(), 1)
        else:
            each(chips, lambda o: g_near(r, o).wait(), 1)
            total = gsrc[r, core, chip].astype(F32) + gin[r, chip].astype(F32)
            for o in range(1, chips):
                total = total + gnear[r, o - 1].astype(F32)
            gkeep[r] = total
            gfar[r] = total.astype(BF16)

            @pl.when(rep != r)
            def _():
                g_far(r).start()

    def tail(r):
        cols = slice(r * width, (r + 1) * width)

        def block_dz(i):
            at = pl.ds(pl.multiple_of(i * block, block), block)
            here = pl.ds(i * groups, groups)
            low = r * per

            def lines(ref, first):
                return jnp.concatenate(
                    [ref[here, first + j:first + j + 1] for j in range(per)], axis=2)

            masked = gs[at, cols].reshape(groups, chunk, width)
            normed = zs[at, cols].reshape(groups, chunk, width)
            dz = (masked - lines(bgath, low) - normed * lines(bgath, half + low)) * lines(fgath, half + low)
            dzs[at, :] = dz.reshape(block, width).astype(BF16)

        each(steps, block_dz)
        acc[...] = jnp.dot(xt[...], dzs[...], preferred_element_type=F32)
        for d in range(ndom):
            gsrc[r, d % cores, d // cores] = acc[d * high:(d + 1) * high, :].astype(BF16)

    for r in range(nrep):
        if r == 0:
            h_stage(2)
        tail(r)
        g_stage(r, 0)
        if r >= 1:
            g_stage(r - 1, 1)
        if r >= 2:
            g_stage(r - 2, 2)
    g_stage(nrep - 1, 1)
    if nrep >= 2:
        g_stage(nrep - 2, 2)
    h_stage(3)
    settle_all(lbuf, lbuf, l_s, l_r)
    losses = lbuf[...]
    source = lax.broadcasted_iota(jnp.int32, losses.shape, 0)
    lane = lax.broadcasted_iota(jnp.int32, losses.shape, 2)
    mine = jnp.sum(jnp.where(lane == me, losses, 0.0), axis=2, keepdims=True)
    loss_out[...] = jnp.sum(jnp.where(lane == source, mine, 0.0), axis=0)[:, :n]
    g_stage(nrep - 1, 2)

    def g_own(o):
        return to(gfar.at[rep], gfarin.at[o], gf_s.at[o], gf_r.at[o], dom, lax.rem(rep + o, nrep))

    each(nrep, lambda o: g_own(o).wait_recv(), 1)
    total = gkeep[rep]
    for o in range(1, nrep):
        total = total + gfarin[o].astype(F32)
    first_out[...] = total
    each(nrep, lambda o: g_own(o).wait_send(), 1)


def hop_kernel(kl, kh, lcols, hcols, adj_l, adj_h, own, halo, out):
    i = pl.program_id(0)
    left = jnp.concatenate([adj_l[0, k] for k in range(kl)] + [adj_h[0, k] for k in range(kh)], axis=1)
    right = jnp.concatenate(
        [own[0, lcols[i, k]] for k in range(kl)] + [halo[hcols[i, k]] for k in range(kh)], axis=0)
    out[0] = jnp.dot(left, right, preferred_element_type=F32).astype(BF16)


def batch_lanes(rows, wide, chunk):
    at = pl.program_id(0) * rows + lax.broadcasted_iota(jnp.int32, (rows, wide), 0)
    return at // chunk == lax.broadcasted_iota(jnp.int32, (rows, wide), 1)


def one_hot(column, count):
    lanes = lax.broadcasted_iota(jnp.int32, (column.shape[0], count), 1)
    return (lanes == column).astype(F32).astype(BF16)


def by_lanes(left, right):
    return lax.dot_general(left, right, (((1,), (1,)), ((), ())), preferred_element_type=F32)


def pick_kernel(chunk, shuf, bound, ids, labels, labelled, feats, x_out, tag_out, sent_out, cnt_out):
    rows = shuf.shape[0]
    nodes = feats.shape[1]
    sent_out[...] = jnp.dot(one_hot(bound[...], nodes), feats[2], preferred_element_type=F32).astype(BF16)
    numbers = ids[...]
    blank = jnp.zeros((6, nodes), F32)
    table = jnp.concatenate(
        [(numbers // 256).astype(F32), (numbers % 256).astype(F32), jnp.zeros((6, ids.shape[1]), F32)], axis=0)
    two = by_lanes(one_hot(shuf[...], ids.shape[1]), table.astype(BF16))
    order = two[:, 0:1] * 256.0 + two[:, 1:2]
    pick = one_hot(order.astype(jnp.int32), nodes)
    whole = jnp.concatenate([feats[0], feats[1], feats[2]], axis=1)
    x_out[...] = jnp.dot(pick, whole, preferred_element_type=F32).astype(BF16)
    marks = jnp.concatenate([labels[...].astype(F32), labelled[...].astype(F32), blank], axis=0)
    tags = by_lanes(pick, marks.astype(BF16))
    tag_out[:, 0:8] = tags
    tag_out[:, 8:9] = order

    @pl.when(pl.program_id(0) == 0)
    def _():
        cnt_out[...] = jnp.zeros_like(cnt_out)

    here = batch_lanes(rows, cnt_out.shape[1], chunk)
    cnt_out[...] += jnp.sum(jnp.where(here, tags[:, 1:2], 0.0), axis=0, keepdims=True)


def emit_kernel(*refs):
    count = len(refs) // 2
    for source, target in zip(refs[:count], refs[count:]):
        target[...] = source[...]


def dma_sems(n, count):
    return [pltpu.SemaphoreType.DMA((n,))] * count


def shards(hop_feats, adj_local, local_cols, adj_halo, halo_cols, boundary_rows, train_ids,
           shuffle, labels, labelled, w_first, w_second):
    ndom, nrep = lax.axis_size("dom"), lax.axis_size("rep")
    n = ndom * nrep
    cores = 2
    row_tiles, kl, tile, _ = adj_local.shape
    kh = adj_halo.shape[1]
    nodes, width = hop_feats.shape[1:]
    slots = train_ids.shape[1]
    hidden_units, classes = w_second.shape[0] * nrep, w_second.shape[1]
    chunk = slots // n
    wide = -(-n // LANES) * LANES
    sds = jax.ShapeDtypeStruct
    own_cols = hidden_units // nrep
    span = -(-classes // LANES) * LANES
    lines = 2 * hidden_units // LANES
    chips = ndom // cores
    peers = chips * nrep
    own_rows, part = 4 * width // ndom, hidden_units // n
    share = boundary_rows.shape[1] // n
    vm = pltpu.VMEM

    def moment_scratch():
        return [vm((n, lines, LANES), F32), vm((chips, nrep, lines, LANES), F32),
                vm((chips, nrep, lines, LANES), F32), vm((peers, lines, LANES), F32), vm((n, lines, LANES), F32)]

    def pairs(a, b, count):
        return [pltpu.SemaphoreType.DMA((a, b))] * count

    grad_block = (own_rows, own_cols)
    half_block = (part, span)
    scratch = [
        vm((8, max(slots, nodes)), jnp.int32), vm((LANES, LANES), F32), vm((slots, LANES), F32),
        vm((nodes, 4 * width), BF16), vm((row_tiles, kl + kh, tile, tile), BF16),
        vm((row_tiles, tile, width), F32), vm((nodes, width), BF16), vm((slots, nodes), BF16),
        vm((n, share, width), BF16), vm((n, share, width), BF16), vm((row_tiles, tile, width), BF16),
        vm((n * share // tile, tile, width), BF16), vm((slots, width), F32),
        vm((nrep, ndom, 4 * width // ndom, own_cols), BF16),
        vm((nrep, ndom, own_cols // ndom, span), BF16),
        vm((span, own_cols), F32), vm((1, 1, wide), F32), vm((n, 1, wide), F32),
    ]
    bands = 4 if row_tiles % 4 == 0 else row_tiles
    scratch += dma_sems(3, 1) + dma_sems(1, 1) + dma_sems(bands, 2) + dma_sems(5, 1) + dma_sems(1, 4)
    scratch += dma_sems(6, 2)
    scratch += [
        vm((slots, 4 * width), BF16), vm((4 * width, slots), BF16), vm((slots, hidden_units), F32),
        vm((slots, hidden_units), F32), vm((slots, own_cols), BF16), vm((hidden_units, span), F32),
        vm((4 * width, own_cols), F32), vm((1, 1, wide), F32), vm((n, 1, wide), F32),
        *moment_scratch(), *moment_scratch(),
        vm((nrep, cores, chips) + grad_block, BF16), vm((nrep, chips) + grad_block, BF16),
        vm((nrep, chips) + grad_block, BF16), vm((nrep, chips - 1) + grad_block, BF16),
        vm((nrep,) + grad_block, BF16), vm((nrep,) + grad_block, F32), vm((nrep,) + grad_block, BF16),
        vm((cores, chips, nrep) + half_block, BF16), vm((chips, nrep) + half_block, BF16),
        vm((chips, nrep) + half_block, BF16), vm((chips - 1, nrep) + half_block, BF16),
        vm((nrep,) + half_block, F32), vm((nrep,) + half_block, BF16), vm((nrep - 1,) + half_block, BF16),
        vm((ndom,) + half_block, F32),
    ]
    moment_sems = dma_sems(1, 5) + dma_sems(chips, 1) + dma_sems(1, 2)
    scratch += moment_sems + moment_sems + dma_sems(1, 2) + dma_sems(nrep, 2)
    scratch += pairs(nrep, chips, 2) + dma_sems(nrep, 2)
    scratch += dma_sems(1, 2) + dma_sems(chips, 2) + dma_sems(nrep, 2) + dma_sems(ndom, 2)
    vmem = pl.BlockSpec(memory_space=pltpu.VMEM)
    smem = pl.BlockSpec(memory_space=pltpu.SMEM)
    where = pl.BlockSpec(memory_space=pl.ANY)
    next_hop, first, second, loss = pl.pallas_call(
        functools.partial(step_kernel, chunk, ndom, nrep, cores, classes, kl, kh),
        out_shape=(sds((nodes, width), BF16), sds((own_rows, own_cols), F32),
                   sds((classes, own_cols), F32), sds((1, n), F32)),
        in_specs=[smem, smem, vmem, vmem] + [where] * 9,
        out_specs=(vmem, vmem, vmem, vmem),
        scratch_shapes=scratch,
        compiler_params=pltpu.CompilerParams(collective_id=2, has_side_effects=True, vmem_limit_bytes=BIG),
        name="step",
    )(local_cols, halo_cols.T, w_first, w_second.T, hop_feats, adj_local, adj_halo,
      hop_feats.reshape(3, row_tiles, tile, width), boundary_rows,
      train_ids, shuffle, labels[None], labelled[None])
    done = (next_hop, loss, first, second)
    specs = [pl.BlockSpec(v.shape, lambda i: (0, 0)) for v in done]
    next_hop, loss, first, second = pl.pallas_call(
        emit_kernel,
        out_shape=tuple(sds(v.shape, v.dtype) for v in done),
        grid=(1,),
        in_specs=specs,
        out_specs=tuple(specs),
        name="emit",
    )(*done)
    return (next_hop, loss, first, second.T)


def solution(mesh):
    both = ("dom", "rep")
    placed = (
        P(None, both, None), P(both, None, None, None), P(both, None), P(both, None, None, None),
        P(both, None), P(both, None), P(both, None), P(both, None), P(both), P(both),
        P(None, "rep"), P("rep", None),
    )
    return jax.shard_map(
        shards, mesh=mesh, in_specs=placed,
        out_specs=(P(both, None), P(both, None), P("dom", "rep"), P("rep", None)),
        check_vma=False,
    )
```

```python
import functools

import jax
import jax.numpy as jnp
from jax import lax
from jax.experimental import pallas as pl
from jax.experimental.pallas import tpu as pltpu
from jax.sharding import PartitionSpec as P

F32 = jnp.float32
BF16 = jnp.bfloat16
BIG = 63 * 1024 * 1024
LANES = 128


def one_hot(column, count):
    lanes = lax.broadcasted_iota(jnp.int32, (column.shape[0], count), 1)
    return (lanes == column).astype(F32).astype(BF16)


def by_lanes(left, right):
    return lax.dot_general(left, right, (((1,), (1,)), ((), ())), preferred_element_type=F32)


def step_kernel(chunk, ndom, nrep, cores, classes, kl, kh,
               lcols, hcols, w1in, w2in, feats, adj_l, adj_h, tiles, bound, ids, shuf, labels, labelled,
               next_out, first_out, second_out, loss_out,
               ints, cols, order, whole, adjv, hacc, nh, pick, sent, halo, own_t, halo_t, tag, w1all, w2all, w2t, crow, cbuf,
               f_s, t_s, a_s, b_s, i_s, c_s, c_r, p_s, p_r, u_s, v_s,
               xs, xt, zs, gs, dzs, g2acc, acc, lrow, lbuf,
               fsrc, fin, fpart, fall, fgath, bsrc, bin_, bpart, ball, bgath,
               gsrc, gin, gsum, gnear, gfar, gkeep, gfarin,
               hsrc, hin, hsum, hnear, hkeep, hfar, hfarin, hgath,
               fx_s, fx_r, fa_s, fa_r, fg_s, fg_r, fw_s, fw_r,
               bx_s, bx_r, ba_s, ba_r, bg_s, bg_r, bw_s, bw_r,
               l_s, l_r, gx_s, gx_r, gn_s, gn_r, gf_s, gf_r,
               hx_s, hx_r, hn_s, hn_r, hf_s, hf_r, hg_s, hg_r):
    n = ndom * nrep
    chips = ndom // cores
    peers = chips * nrep
    dom, rep = lax.axis_index("dom"), lax.axis_index("rep")
    me = dom * nrep + rep
    chip, core = dom // cores, lax.rem(dom, cores)
    other = cores - 1 - core
    block = 256
    slots, hidden_units = zs.shape
    steps = slots // block
    groups = block // chunk
    half = fsrc.shape[1] // 2
    width = hidden_units // nrep
    per = half // nrep

    barrier = pltpu.get_barrier_semaphore()

    def greet(o, carry):
        peer = lax.rem(me + o, n)
        pl.semaphore_signal(barrier, inc=1, device_id=(peer // nrep, lax.rem(peer, nrep)),
                            device_id_type=pl.DeviceIdType.MESH)
        return carry

    lax.fori_loop(1, n, greet, 0)

    def to(src, dst, ssem, rsem, peer_dom, peer_rep):
        return pltpu.make_async_remote_copy(
            src_ref=src, dst_ref=dst, send_sem=ssem, recv_sem=rsem,
            device_id=(peer_dom, peer_rep), device_id_type=pl.DeviceIdType.MESH)

    def each(count, fn, first=0):
        lax.fori_loop(first, count, lambda i, carry: (fn(i), carry)[1], 0)

    def group_of(a, c):
        return pl.ds((a * cores + c) * nrep, nrep)

    def plane(o):
        return lax.rem(chip + o, chips)

    def rows_of(i):
        return pl.ds(pl.multiple_of(i * block, block), block)

    row_tiles, tile, fw = hacc.shape
    nodes = whole.shape[0]

    def feat_copy(k):
        return pltpu.make_async_copy(feats.at[k], whole.at[:, k * fw:(k + 1) * fw], f_s.at[k])

    bands = a_s.shape[0]
    deep = row_tiles // bands

    def near_copy(j):
        at = pl.ds(j * deep, deep)
        return pltpu.make_async_copy(adj_l.at[at], adjv.at[at, 0:kl], a_s.at[j])

    def far_copy(j):
        at = pl.ds(j * deep, deep)
        return pltpu.make_async_copy(adj_h.at[at], adjv.at[at, kl:kl + kh], b_s.at[j])

    given = (shuf, ids, labels, labelled, bound)
    int_copies = [pltpu.make_async_copy(ref, ints.at[m:m + 1, 0:ref.shape[1]], i_s.at[m])
                  for m, ref in enumerate(given)]
    for copy in int_copies:
        copy.start()
    own_copy = pltpu.make_async_copy(tiles.at[2], own_t, t_s.at[0])
    own_copy.start()
    feat_copy(2).start()
    feat_copy(0).start()
    feat_copy(1).start()
    each(bands, lambda j: near_copy(j).start())
    each(bands, lambda j: far_copy(j).start())

    w1all[rep] = w1in[...].reshape(w1all.shape[1:])
    w2t[...] = jnp.zeros_like(w2t)
    w2t[0:classes, :] = w2in[...].astype(F32)
    w2all[rep] = w2t[...].T.astype(BF16).reshape(w2all.shape[1:])
    for copy in int_copies:
        copy.wait()

    def lines_of(m, count):
        return jnp.concatenate([ints[m:m + 1, j * LANES:(j + 1) * LANES] for j in range(count)], axis=0)

    per_slot, per_node, per_bound = slots // LANES, nodes // LANES, bound.shape[1] // LANES
    shuf_lines, id_lines = lines_of(0, per_slot), lines_of(1, per_slot)
    stack = [shuf_lines % LANES, shuf_lines // LANES, id_lines // LANES, id_lines % LANES,
             lines_of(2, per_node), lines_of(3, per_node), lines_of(4, per_bound)]
    used = sum(s.shape[0] for s in stack)
    stack = jnp.concatenate(stack + [jnp.zeros((LANES - used, LANES), jnp.int32)], axis=0)
    turned = stack.astype(F32).T
    cols[...] = turned

    def column(m):
        return cols[:, m:m + 1]

    at_bound = 2 * per_slot + 2 * per_slot + 2 * per_node
    own_copy.wait()
    last = own_t[...].reshape(nodes, fw)
    share = sent.shape[1]
    for m in range(per_bound):
        spot = one_hot(column(at_bound + m).astype(jnp.int32), nodes)
        rows = jnp.dot(spot, last, preferred_element_type=F32)
        count = LANES // share
        sent[m * count:(m + 1) * count] = rows.reshape(count, share, fw).astype(BF16)
    lane = lax.broadcasted_iota(jnp.int32, (LANES, LANES), 1).astype(F32)
    table = cols[:, 2 * per_slot:4 * per_slot].astype(BF16)
    pair = lax.broadcasted_iota(jnp.int32, (LANES, 2 * per_slot), 1).astype(F32)
    for k in range(per_slot):
        low = (lane == column(k)).astype(F32).astype(BF16)
        found = jnp.dot(low, table, preferred_element_type=F32)
        high = column(per_slot + k)
        value = jnp.where(pair == high, found * LANES, jnp.where(pair == high + per_slot, found, 0.0))
        order[k * LANES:(k + 1) * LANES, 0:1] = jnp.sum(value, axis=1, keepdims=True)
    for k in range(per_node):
        marks = jnp.where(lane == 0, column(4 * per_slot + k),
                          jnp.where(lane == 1, column(4 * per_slot + per_node + k), 0.0))
        whole[k * LANES:(k + 1) * LANES, 3 * fw:4 * fw] = marks.astype(BF16)
    for k in range(3):
        feat_copy(k).wait()

    def batch_rows(i, count):
        rows_at = i * count + lax.broadcasted_iota(jnp.int32, (count, crow.shape[2]), 0)
        return rows_at // chunk == lax.broadcasted_iota(jnp.int32, (count, crow.shape[2]), 1)

    def gather_rows(i, own):
        at = rows_of(i)
        spot = order[at, 0:1].astype(jnp.int32)
        strip = 2 * LANES
        for j in range(nodes // strip):
            pick[at, j * strip:(j + 1) * strip] = one_hot(spot - j * strip, strip)
        rows = jnp.dot(pick[at, :], whole[...], preferred_element_type=F32)
        xs[at, 0:3 * fw] = rows[:, 0:3 * fw].astype(BF16)
        tags = rows[:, 3 * fw:4 * fw]
        tag[at, :] = tags
        return own + jnp.sum(jnp.where(batch_rows(i, block), tags[:, 1:2], 0.0), axis=0, keepdims=True)

    early = 0
    own_counts = lax.fori_loop(0, early, gather_rows, jnp.zeros((1, crow.shape[2]), F32))
    pl.semaphore_wait(barrier, n - 1)

    def send_halo(o):
        peer = lax.rem(me + o, n)
        return to(sent.at[peer], halo.at[me], p_s.at[0], p_r.at[0], peer // nrep, lax.rem(peer, nrep))

    def settle_all(src, dst, ssem, rsem):
        to(src.at[pl.ds(0, n - 1)], dst.at[pl.ds(0, n - 1)], ssem.at[0], rsem.at[0],
           chip * cores + other, rep).wait()

    def spread_weights(buf, sems):
        zsem, zrec, psem, prec, csem, crec = [sems.at[k] for k in range(6)]

        def along(o):
            return to(buf.at[rep, dom], buf.at[rep, dom], zsem, zrec, dom, lax.rem(rep + o, nrep))

        def across(p, o):
            at = lax.rem(rep + o, nrep)
            return to(buf.at[at, dom], buf.at[at, dom], psem, prec, plane(p) * cores + core, rep)

        def swap(p, o):
            at = lax.rem(rep + o, nrep)
            src = buf.at[at, lax.rem(chip - p + chips, chips) * cores + core]
            return to(src, src, csem, crec, chip * cores + other, rep)

        def each_pair(first, fn):
            each(chips, lambda p: each(nrep, lambda o: fn(p, o), 1), first)

        def settle(count, ssem, rsem):
            if count <= ndom:
                ref = buf.at[0, pl.ds(0, count)]
            else:
                ref = buf.at[pl.ds(0, nrep - 1), pl.ds(0, count // (nrep - 1))]
            to(ref, ref, ssem, rsem, chip * cores + other, rep).wait()

        def stage(s):
            if s == 0:
                each(nrep, lambda o: along(o).start(), 1)
            elif s == 1:
                settle(nrep - 1, zsem, zrec)
                each_pair(1, lambda p, o: across(p, o).start())
            elif s == 2:
                settle((nrep - 1) * (chips - 1), psem, prec)
                each_pair(0, lambda p, o: swap(p, o).start())
            else:
                settle((nrep - 1) * chips, csem, crec)
        return stage

    w1_stage = spread_weights(w1all, u_s)
    w2_stage = spread_weights(w2all, v_s)
    each(n, lambda o: send_halo(o).start(), 1)
    w1_stage(0)
    w2_stage(0)
    halo[me] = sent[me]

    own_counts = lax.fori_loop(early, steps, gather_rows, own_counts)
    w1_stage(1)
    crow[0] = own_counts
    cbuf[me] = own_counts

    def send_count(o):
        peer = lax.rem(me + o, n)
        return to(crow.at[0], cbuf.at[me], c_s.at[0], c_r.at[0], peer // nrep, lax.rem(peer, nrep))

    each(n, lambda o: send_count(o).start(), 1)

    def hop_near(i):
        left = jnp.concatenate([adjv[i, k] for k in range(kl)], axis=1)
        right = jnp.concatenate([own_t[lcols[i, k]] for k in range(kl)], axis=0)
        hacc[i] = jnp.dot(left, right, preferred_element_type=F32)

    def near_band(j):
        near_copy(j).wait()
        each((j + 1) * deep, hop_near, j * deep)

    each(bands, near_band)
    settle_all(sent, halo, p_s, p_r)
    halo_t[...] = halo[...].reshape(halo_t.shape)

    each(bands, lambda j: far_copy(j).wait())

    def hop_far(i):
        left = jnp.concatenate([adjv[i, kl + k] for k in range(kh)], axis=1)
        right = jnp.concatenate(
            [halo_t[hcols[k, i]] for k in range(kh)], axis=0)
        total = (hacc[i] + jnp.dot(left, right, preferred_element_type=F32)).astype(BF16)
        nh[pl.ds(pl.multiple_of(i * tile, tile), tile), :] = total
        next_out[pl.ds(pl.multiple_of(i * tile, tile), tile), :] = total

    each(row_tiles, hop_far)
    w1_stage(2)
    w2_stage(1)

    def gather_next(i):
        at = rows_of(i)
        xs[at, 3 * fw:4 * fw] = jnp.dot(pick[at, :], nh[...], preferred_element_type=F32).astype(BF16)

    each(steps, gather_next)
    w1_stage(3)

    def pre(i):
        at = rows_of(i)
        here = pl.ds(i * groups, groups)
        x = xs[at, :]
        for r in range(nrep):
            w1 = w1all[r].reshape(w1in.shape)
            z = jnp.dot(x, w1, preferred_element_type=F32)
            zs[at, r * width:(r + 1) * width] = z
            z3 = z.reshape(groups, chunk, width)
            mean = jnp.sum(z3, axis=1, keepdims=True) * (1.0 / chunk)
            off = z3 - mean
            spread2 = jnp.sum(off * off, axis=1, keepdims=True)
            for j in range(per):
                cut = slice(j * 128, (j + 1) * 128)
                fsrc[here, r * per + j:r * per + j + 1] = mean[:, :, cut]
                fsrc[here, half + r * per + j:half + r * per + j + 1] = spread2[:, :, cut]

    each(steps, pre)
    w2_stage(2)

    def chip_sum(src, got, part, xs_, xr, combine):
        def swap(a):
            return to(src.at[group_of(a, other)], got.at[a], xs_.at[0], xr.at[0], chip * cores + other, rep)

        def start():
            each(chips, lambda a: swap(a).start())

        def finish():
            to(part, got, xs_.at[0], xr.at[0], chip * cores + other, rep).wait()

            def one(a):
                part[a] = combine(src[group_of(a, core)], got[a])
            each(chips, one)
        return start, finish

    def walk(o):
        return lax.rem(chip + o // nrep, chips), lax.rem(rep + lax.rem(o, nrep), nrep)

    def scatter(part, arrived, as_, ar):
        def copy(o):
            a, r = walk(o)
            return to(part.at[a, r], arrived.at[o], as_.at[0], ar.at[0], a * cores + core, r)

        def start():
            each(peers, lambda o: copy(o).start(), 1)
            arrived[0] = part[chip, rep]

        def finish():
            span = arrived.at[pl.ds(0, peers - 1)]
            to(span, span, as_.at[0], ar.at[0], chip * cores + other, rep).wait()
        return start, finish

    def gather(gath, gs_, gr, ws, wr):
        def copy(o):
            a, r = walk(o)
            return to(gath.at[me], gath.at[me], gs_.at[0], gr.at[o // nrep], a * cores + core, r)

        def forward(da):
            at = group_of(lax.rem(chip + chips - da, chips), core)
            return to(gath.at[at], gath.at[at], ws.at[0], wr.at[0], chip * cores + other, rep)

        def settle(count, ssem, rsem):
            span = gath.at[pl.ds(0, count)]
            return to(span, span, ssem, rsem, chip * cores + other, rep)

        def start():
            each(peers, lambda o: copy(o).start(), 1)

        def finish():
            settle(nrep - 1, gs_.at[0], gr.at[0]).wait_recv()
            forward(0).start()

            def chip_in(da):
                settle(nrep, gs_.at[0], gr.at[da]).wait_recv()
                forward(da).start()
            each(chips, chip_in, 1)
            settle(peers, ws.at[0], wr.at[0]).wait()
            settle(peers - 1, gs_.at[0], gr.at[0]).wait_send()
        return start, finish

    def both_moments(a, b):
        ma, mb = a[:, :half], b[:, :half]
        gap = ma - mb
        spread2 = a[:, half:] + b[:, half:] + (0.5 * chunk) * gap * gap
        return jnp.concatenate([(ma + mb) * 0.5, spread2], axis=1)

    start, finish = chip_sum(fsrc, fin, fpart, fx_s, fx_r, both_moments)
    start()
    each(steps, lambda i: xt.__setitem__(
        (slice(None), pl.ds(pl.multiple_of(i * block, block), block)),
        xs[pl.ds(pl.multiple_of(i * block, block), block), :].T))
    finish()
    start, finish = scatter(fpart, fall, fa_s, fa_r)
    start()
    finish()
    got = fall[...]
    mu = jnp.sum(got[:, :half], axis=0) * (1.0 / peers)
    off = got[:, :half] - mu[None]
    m2 = jnp.sum(got[:, half:], axis=0) + (cores * chunk) * jnp.sum(off * off, axis=0)
    fgath[me] = jnp.concatenate([mu, lax.rsqrt(m2 * (1.0 / (n * chunk)) + 1e-05)], axis=0)
    start, finish = gather(fgath, fg_s, fg_r, fw_s, fw_r)
    start()
    loss_row = jnp.zeros((1, lrow.shape[2]), F32)
    w2_stage(3)
    settle_all(cbuf, cbuf, c_s, c_r)
    counts = jnp.maximum(jnp.sum(cbuf[...], axis=0), 1.0)
    finish()


    few = block
    some = few // chunk

    def head_rows(i):
        at = pl.ds(pl.multiple_of(i * few, few), few)
        here = pl.ds(i * some, some)
        st = fgath[here]
        for r in range(nrep):
            span = slice(r * width, (r + 1) * width)
            z3 = zs[at, span].reshape(some, chunk, width)
            mean = jnp.concatenate([st[:, r * per + j:r * per + j + 1] for j in range(per)], axis=2)
            rstd = jnp.concatenate(
                [st[:, half + r * per + j:half + r * per + j + 1] for j in range(per)], axis=2)
            normed = ((z3 - mean) * rstd).reshape(few, width)
            zs[at, span] = normed
            pick[at, span] = jnp.maximum(normed, 0.0).astype(BF16)
        second = w2all[...].reshape(hidden_units, w2all.shape[3])
        logits = jnp.dot(pick[at, 0:hidden_units], second, preferred_element_type=F32)
        lane = lax.broadcasted_iota(jnp.int32, logits.shape, 1)
        logits = jnp.where(lane < classes, logits, -1e30)
        row_max = jnp.max(logits, axis=1, keepdims=True)
        expos = jnp.exp(logits - row_max)
        totals = jnp.sum(expos, axis=1, keepdims=True)
        target = tag[at, 0:1].astype(jnp.int32)
        mark = tag[at, 1:2]
        onehot = (lane == target).astype(F32)
        cross = jnp.log(totals) + row_max - jnp.sum(onehot * logits, axis=1, keepdims=True)
        mine = batch_rows(i, few)
        count = jnp.sum(jnp.where(mine, counts, 0.0), axis=1, keepdims=True)
        dlogits = ((expos / totals - onehot) * (mark / count)).astype(BF16)
        pick[at, hidden_units:hidden_units + dlogits.shape[1]] = dlogits
        for r in range(nrep):
            span = slice(r * width, (r + 1) * width)
            seen = zs[at, span]
            back = by_lanes(dlogits, w2all[r].reshape(width, w2all.shape[3]))
            masked = jnp.where(seen > 0, back, 0.0)
            gs[at, span] = masked
            sums = jnp.sum(masked.reshape(some, chunk, width), axis=1, keepdims=True)
            projs = jnp.sum((masked * seen).reshape(some, chunk, width), axis=1, keepdims=True)
            for j in range(per):
                cut = slice(j * 128, (j + 1) * 128)
                bsrc[here, r * per + j:r * per + j + 1] = sums[:, :, cut]
                bsrc[here, half + r * per + j:half + r * per + j + 1] = projs[:, :, cut]
        return jnp.sum(jnp.where(mine, mark * cross, 0.0), axis=0, keepdims=True)

    def head(i, loss_row):
        for k in range(block // few):
            loss_row = loss_row + head_rows(i * (block // few) + k)
        return loss_row

    loss_row = lax.fori_loop(0, steps, head, loss_row)
    start, finish = chip_sum(bsrc, bin_, bpart, bx_s, bx_r, lambda a, b: a + b)
    start()
    loss_row = loss_row / jnp.maximum(own_counts, 1.0)
    lrow[0] = loss_row
    lbuf[me] = loss_row

    def send_loss(o):
        peer = lax.rem(me + o, n)
        return to(lrow.at[0], lbuf.at[me], l_s.at[0], l_r.at[0], peer // nrep, lax.rem(peer, nrep))

    part = hsrc.shape[3]
    for r in range(nrep):
        g2acc[r * width:(r + 1) * width, :] = lax.dot_general(
            pick[:, r * width:(r + 1) * width], pick[:, hidden_units:hidden_units + g2acc.shape[1]],
            (((0,), (0,)), ((), ())), preferred_element_type=F32)
        for d in range(ndom):
            first_row = (r * ndom + d) * part
            hsrc[d % cores, d // cores, r] = g2acc[first_row:first_row + part, :].astype(BF16)
    def h_near(o):
        return to(hsum.at[plane(o)], hnear.at[o - 1], hn_s.at[o], hn_r.at[o], plane(o) * cores + core, rep)

    def h_along(o):
        peer = lax.rem(rep + o, nrep)
        return to(hfar.at[peer], hfarin.at[o - 1], hf_s.at[o], hf_r.at[o], dom, peer)

    def h_round(o):
        return to(hgath.at[dom], hgath.at[dom], hg_s.at[o], hg_r.at[o], lax.rem(dom + o, ndom), rep)

    def h_stage(stage):
        if stage == 0:
            each(chips, lambda o: h_near(o).start(), 1)
        elif stage == 1:
            each(chips, lambda o: h_near(o).wait(), 1)
            total = hsrc[core, chip].astype(F32) + hin[chip].astype(F32)
            for o in range(1, chips):
                total = total + hnear[o - 1].astype(F32)
            hkeep[...] = total
            hfar[...] = total.astype(BF16)
            each(nrep, lambda o: h_along(o).start(), 1)
        elif stage == 2:
            each(nrep, lambda o: h_along(o).wait(), 1)
            total = hkeep[rep]
            for o in range(1, nrep):
                total = total + hfarin[o - 1].astype(F32)
            hgath[dom] = total
            each(ndom, lambda o: h_round(o).start(), 1)
        else:
            each(ndom, lambda o: h_round(o).wait(), 1)
            both = hgath[...].reshape(ndom * part, hgath.shape[2]).T
            second_out[...] = both[:classes]

    h_swap = to(hsrc.at[other], hin, hx_s.at[0], hx_r.at[0], chip * cores + other, rep)
    h_swap.start()
    finish()
    start, finish = scatter(bpart, ball, ba_s, ba_r)
    start()
    h_swap.wait()
    hsum[...] = (hsrc[core].astype(F32) + hin[...].astype(F32)).astype(BF16)
    h_stage(0)
    finish()
    bgath[me] = jnp.sum(ball[...], axis=0) * (1.0 / (n * chunk))
    start, finish = gather(bgath, bg_s, bg_r, bw_s, bw_r)
    start()
    each(n, lambda o: send_loss(o).start(), 1)
    h_stage(1)
    finish()

    high = acc.shape[0] // ndom

    def g_swap(r):
        return to(gsrc.at[r, other], gin.at[r], gx_s.at[r], gx_r.at[r], chip * cores + other, rep)

    def g_near(r, o):
        return to(gsum.at[r, plane(o)], gnear.at[r, o - 1], gn_s.at[r, o], gn_r.at[r, o],
                  plane(o) * cores + core, rep)

    def g_far(r):
        o = lax.rem(r - rep + nrep, nrep)
        return to(gfar.at[r], gfarin.at[o], gf_s.at[o], gf_r.at[o], dom, r)

    def g_stage(r, stage):
        if stage == 0:
            g_swap(r).start()
        elif stage == 1:
            g_swap(r).wait()
            gsum[r] = (gsrc[r, core].astype(F32) + gin[r].astype(F32)).astype(BF16)
            each(chips, lambda o: g_near(r, o).start(), 1)
        else:
            each(chips, lambda o: g_near(r, o).wait(), 1)
            total = gsrc[r, core, chip].astype(F32) + gin[r, chip].astype(F32)
            for o in range(1, chips):
                total = total + gnear[r, o - 1].astype(F32)
            gkeep[r] = total
            gfar[r] = total.astype(BF16)

            @pl.when(rep != r)
            def _():
                g_far(r).start()

    def tail(r):
        cols = slice(r * width, (r + 1) * width)

        def block_dz(i):
            at = pl.ds(pl.multiple_of(i * block, block), block)
            here = pl.ds(i * groups, groups)
            low = r * per

            def lines(ref, first):
                return jnp.concatenate(
                    [ref[here, first + j:first + j + 1] for j in range(per)], axis=2)

            masked = gs[at, cols].reshape(groups, chunk, width)
            normed = zs[at, cols].reshape(groups, chunk, width)
            dz = (masked - lines(bgath, low) - normed * lines(bgath, half + low)) * lines(fgath, half + low)
            dzs[at, :] = dz.reshape(block, width).astype(BF16)

        each(steps, block_dz)
        acc[...] = jnp.dot(xt[...], dzs[...], preferred_element_type=F32)
        for d in range(ndom):
            gsrc[r, d % cores, d // cores] = acc[d * high:(d + 1) * high, :].astype(BF16)

    for r in range(nrep):
        if r == 0:
            h_stage(2)
        tail(r)
        g_stage(r, 0)
        if r >= 1:
            g_stage(r - 1, 1)
        if r >= 2:
            g_stage(r - 2, 2)
    g_stage(nrep - 1, 1)
    if nrep >= 2:
        g_stage(nrep - 2, 2)
    h_stage(3)
    settle_all(lbuf, lbuf, l_s, l_r)
    losses = lbuf[...]
    source = lax.broadcasted_iota(jnp.int32, losses.shape, 0)
    lane = lax.broadcasted_iota(jnp.int32, losses.shape, 2)
    mine = jnp.sum(jnp.where(lane == me, losses, 0.0), axis=2, keepdims=True)
    loss_out[...] = jnp.sum(jnp.where(lane == source, mine, 0.0), axis=0)[:, :n]
    g_stage(nrep - 1, 2)

    def g_own(o):
        return to(gfar.at[rep], gfarin.at[o], gf_s.at[o], gf_r.at[o], dom, lax.rem(rep + o, nrep))

    each(nrep, lambda o: g_own(o).wait_recv(), 1)
    total = gkeep[rep]
    for o in range(1, nrep):
        total = total + gfarin[o].astype(F32)
    first_out[...] = total
    each(nrep, lambda o: g_own(o).wait_send(), 1)


def hop_kernel(kl, kh, lcols, hcols, adj_l, adj_h, own, halo, out):
    i = pl.program_id(0)
    left = jnp.concatenate([adj_l[0, k] for k in range(kl)] + [adj_h[0, k] for k in range(kh)], axis=1)
    right = jnp.concatenate(
        [own[0, lcols[i, k]] for k in range(kl)] + [halo[hcols[i, k]] for k in range(kh)], axis=0)
    out[0] = jnp.dot(left, right, preferred_element_type=F32).astype(BF16)


def batch_lanes(rows, wide, chunk):
    at = pl.program_id(0) * rows + lax.broadcasted_iota(jnp.int32, (rows, wide), 0)
    return at // chunk == lax.broadcasted_iota(jnp.int32, (rows, wide), 1)


def one_hot(column, count):
    lanes = lax.broadcasted_iota(jnp.int32, (column.shape[0], count), 1)
    return (lanes == column).astype(F32).astype(BF16)


def by_lanes(left, right):
    return lax.dot_general(left, right, (((1,), (1,)), ((), ())), preferred_element_type=F32)


def pick_kernel(chunk, shuf, bound, ids, labels, labelled, feats, x_out, tag_out, sent_out, cnt_out):
    rows = shuf.shape[0]
    nodes = feats.shape[1]
    sent_out[...] = jnp.dot(one_hot(bound[...], nodes), feats[2], preferred_element_type=F32).astype(BF16)
    numbers = ids[...]
    blank = jnp.zeros((6, nodes), F32)
    table = jnp.concatenate(
        [(numbers // 256).astype(F32), (numbers % 256).astype(F32), jnp.zeros((6, ids.shape[1]), F32)], axis=0)
    two = by_lanes(one_hot(shuf[...], ids.shape[1]), table.astype(BF16))
    order = two[:, 0:1] * 256.0 + two[:, 1:2]
    pick = one_hot(order.astype(jnp.int32), nodes)
    whole = jnp.concatenate([feats[0], feats[1], feats[2]], axis=1)
    x_out[...] = jnp.dot(pick, whole, preferred_element_type=F32).astype(BF16)
    marks = jnp.concatenate([labels[...].astype(F32), labelled[...].astype(F32), blank], axis=0)
    tags = by_lanes(pick, marks.astype(BF16))
    tag_out[:, 0:8] = tags
    tag_out[:, 8:9] = order

    @pl.when(pl.program_id(0) == 0)
    def _():
        cnt_out[...] = jnp.zeros_like(cnt_out)

    here = batch_lanes(rows, cnt_out.shape[1], chunk)
    cnt_out[...] += jnp.sum(jnp.where(here, tags[:, 1:2], 0.0), axis=0, keepdims=True)


def emit_kernel(*refs):
    count = len(refs) // 2
    for source, target in zip(refs[:count], refs[count:]):
        target[...] = source[...]


def dma_sems(n, count):
    return [pltpu.SemaphoreType.DMA((n,))] * count


def shards(hop_feats, adj_local, local_cols, adj_halo, halo_cols, boundary_rows, train_ids,
           shuffle, labels, labelled, w_first, w_second):
    ndom, nrep = lax.axis_size("dom"), lax.axis_size("rep")
    n = ndom * nrep
    cores = 2
    row_tiles, kl, tile, _ = adj_local.shape
    kh = adj_halo.shape[1]
    nodes, width = hop_feats.shape[1:]
    slots = train_ids.shape[1]
    hidden_units, classes = w_second.shape[0] * nrep, w_second.shape[1]
    chunk = slots // n
    wide = -(-n // LANES) * LANES
    sds = jax.ShapeDtypeStruct
    own_cols = hidden_units // nrep
    span = -(-classes // LANES) * LANES
    lines = 2 * hidden_units // LANES
    chips = ndom // cores
    peers = chips * nrep
    own_rows, part = 4 * width // ndom, hidden_units // n
    share = boundary_rows.shape[1] // n
    vm = pltpu.VMEM

    def moment_scratch():
        return [vm((n, lines, LANES), F32), vm((chips, nrep, lines, LANES), F32),
                vm((chips, nrep, lines, LANES), F32), vm((peers, lines, LANES), F32), vm((n, lines, LANES), F32)]

    def pairs(a, b, count):
        return [pltpu.SemaphoreType.DMA((a, b))] * count

    grad_block = (own_rows, own_cols)
    half_block = (part, span)
    scratch = [
        vm((8, max(slots, nodes)), jnp.int32), vm((LANES, LANES), F32), vm((slots, LANES), F32),
        vm((nodes, 4 * width), BF16), vm((row_tiles, kl + kh, tile, tile), BF16),
        vm((row_tiles, tile, width), F32), vm((nodes, width), BF16), vm((slots, nodes), BF16),
        vm((n, share, width), BF16), vm((n, share, width), BF16), vm((row_tiles, tile, width), BF16),
        vm((n * share // tile, tile, width), BF16), vm((slots, width), F32),
        vm((nrep, ndom, 4 * width // ndom, own_cols), BF16),
        vm((nrep, ndom, own_cols // ndom, span), BF16),
        vm((span, own_cols), F32), vm((1, 1, wide), F32), vm((n, 1, wide), F32),
    ]
    bands = 4 if row_tiles % 4 == 0 else row_tiles
    scratch += dma_sems(3, 1) + dma_sems(1, 1) + dma_sems(bands, 2) + dma_sems(5, 1) + dma_sems(1, 4)
    scratch += dma_sems(6, 2)
    scratch += [
        vm((slots, 4 * width), BF16), vm((4 * width, slots), BF16), vm((slots, hidden_units), F32),
        vm((slots, hidden_units), F32), vm((slots, own_cols), BF16), vm((hidden_units, span), F32),
        vm((4 * width, own_cols), F32), vm((1, 1, wide), F32), vm((n, 1, wide), F32),
        *moment_scratch(), *moment_scratch(),
        vm((nrep, cores, chips) + grad_block, BF16), vm((nrep, chips) + grad_block, BF16),
        vm((nrep, chips) + grad_block, BF16), vm((nrep, chips - 1) + grad_block, BF16),
        vm((nrep,) + grad_block, BF16), vm((nrep,) + grad_block, F32), vm((nrep,) + grad_block, BF16),
        vm((cores, chips, nrep) + half_block, BF16), vm((chips, nrep) + half_block, BF16),
        vm((chips, nrep) + half_block, BF16), vm((chips - 1, nrep) + half_block, BF16),
        vm((nrep,) + half_block, F32), vm((nrep,) + half_block, BF16), vm((nrep - 1,) + half_block, BF16),
        vm((ndom,) + half_block, F32),
    ]
    moment_sems = dma_sems(1, 5) + dma_sems(chips, 1) + dma_sems(1, 2)
    scratch += moment_sems + moment_sems + dma_sems(1, 2) + dma_sems(nrep, 2)
    scratch += pairs(nrep, chips, 2) + dma_sems(nrep, 2)
    scratch += dma_sems(1, 2) + dma_sems(chips, 2) + dma_sems(nrep, 2) + dma_sems(ndom, 2)
    vmem = pl.BlockSpec(memory_space=pltpu.VMEM)
    smem = pl.BlockSpec(memory_space=pltpu.SMEM)
    where = pl.BlockSpec(memory_space=pl.ANY)
    next_hop, first, second, loss = pl.pallas_call(
        functools.partial(step_kernel, chunk, ndom, nrep, cores, classes, kl, kh),
        out_shape=(sds((nodes, width), BF16), sds((own_rows, own_cols), F32),
                   sds((classes, own_cols), F32), sds((1, n), F32)),
        in_specs=[smem, smem, vmem, vmem] + [where] * 9,
        out_specs=(vmem, vmem, vmem, vmem),
        scratch_shapes=scratch,
        compiler_params=pltpu.CompilerParams(collective_id=2, has_side_effects=True, vmem_limit_bytes=BIG),
        name="step",
    )(local_cols, halo_cols.T, w_first, w_second.T, hop_feats, adj_local, adj_halo,
      hop_feats.reshape(3, row_tiles, tile, width), boundary_rows,
      train_ids, shuffle, labels[None], labelled[None])
    done = (next_hop, loss, first, second)
    specs = [pl.BlockSpec(v.shape, lambda i: (0, 0)) for v in done]
    next_hop, loss, first, second = pl.pallas_call(
        emit_kernel,
        out_shape=tuple(sds(v.shape, v.dtype) for v in done),
        grid=(1,),
        in_specs=specs,
        out_specs=tuple(specs),
        name="emit",
    )(*done)
    return (next_hop, loss, first, second.T)


def solution(mesh):
    both = ("dom", "rep")
    placed = (
        P(None, both, None), P(both, None, None, None), P(both, None), P(both, None, None, None),
        P(both, None), P(both, None), P(both, None), P(both, None), P(both), P(both),
        P(None, "rep"), P("rep", None),
    )
    return jax.shard_map(
        shards, mesh=mesh, in_specs=placed,
        out_specs=(P(both, None), P(both, None), P("dom", "rep"), P("rep", None)),
        check_vma=False,
    )
```
